32 devices in a mesh: tensor: 4 (over y, core), expert: 4 (over z), dp: 2 (over x).
Axes of the slice: x: 2, y: 2, z: 4, core: 2. Of those that a mesh axis runs over, the one named last changes fastest.
Arguments:
- grad_out: bfloat16 [512, 4096], P(('expert', 'dp')), may hold values from -6 to 6
- route_ids: int32 [512, 8], P(('expert', 'dp')), may hold values from 0 to 127, all different within a row; in each aligned block of 64 rows (0 to 63, 64 to 127, ...) at most 6 rows name the same one
- route_probs: bfloat16 [512, 8], P(('expert', 'dp')), may hold values from 0.019897461 to 0.5
- gate_act: bfloat16 [2, 128, 24, 768], P('dp', 'expert', None, 'tensor'), may hold values from -8 to 8
- up_act: bfloat16 [2, 128, 24, 768], P('dp', 'expert', None, 'tensor'), may hold values from -6 to 6
- w_down: bfloat16 [128, 768, 4096], P('expert', 'tensor'), may hold values from -0.21875 to 0.21875
Outputs:
- grad_gate: bfloat16 [2, 128, 24, 768], P('dp', 'expert', None, 'tensor')
- grad_up: bfloat16 [2, 128, 24, 768], P('dp', 'expert', None, 'tensor')
- grad_w_down: bfloat16 [128, 768, 4096], P('expert', 'tensor', 'dp')
- grad_probs: float32 [512, 8], P(('expert', 'dp'))
The draws below stay inside these ranges and needn't reach their ends.
Inputs may be any that keep to these rules, and one draw needn't show every extreme that they name: `route_ids`: each row names 8 different experts. Within the 64 rows of one index pair of expert and dp no expert is named more than 6 times, and in every draw some expert is named exactly 6 times there.
All inputs are finite; a program needn't handle non-finite values.
Results may differ from the reference program's by a relative error of at most 0.009.
Values may be sent and summed in bfloat16 or wider, within the bound.
A program may use at most 192 MiB of HBM per device.

```python
import math
import jax
import jax.numpy as jnp
import numpy as np
from jax import lax

D = 4096
FF = 768
EXPERTS = 128
TOP = 8
TOK_DEV = 64
CAP = 6
SLOTS = 24
TOKENS = 512
N_EXPERT = 4
N_DP = 2


def shard_levels(own_key, extent, split, smallest, top_value):
    def one(axis_at, shards_of):
        heights = jax.random.uniform(jax.random.fold_in(jax.random.fold_in(own_key, 6), axis_at), (shards_of,), jnp.float32, smallest / len(split), top_value / len(split))
        return jnp.repeat(jnp.exp(heights), extent[axis_at] // shards_of).reshape((-1,) + (1,) * (len(extent) - axis_at - 1))

    level = one(*split[0])
    for cut in split[1:]:
        level = level * one(*cut)
    return level


def assign_block(rng, own, number, rows, count, top, most, skew):
    order = jax.random.permutation(rng, count)
    packed, ordinary = shares(count, rows * top, most, skew, True), shares(count, rows * top, most, skew, False)
    places = jnp.arange(count)

    def named(lengths, offset_by):
        used = int((lengths > 0).sum())
        fixed = max(1, used // 4)
        passed = fixed + (places - fixed + offset_by * (used - fixed)) % max(1, count - fixed)
        return jnp.zeros((count,), jnp.int32).at[order[jnp.where(places < fixed, places, passed)]].set(jnp.asarray(lengths, jnp.int32))

    lengths = jnp.where(number % 4 == 0, named(packed, number // 4), named(ordinary, number - number // 4 - 1))
    mixed = jax.random.permutation(jax.random.fold_in(own, 3), count)
    donor, receiver = mixed[0:count // 2 * 2:2], mixed[1:count // 2 * 2:2]
    room = jnp.minimum(lengths[donor] - 1, most - lengths[receiver]) // 2
    room = jnp.where((donor == order[0]) | (receiver == order[0]) | (lengths[receiver] == 0), 0, jnp.maximum(room, 0))
    passed = jax.random.randint(jax.random.fold_in(own, 4), (count // 2,), 0, 1 << 20) % (room + 1)
    lengths = lengths.at[donor].add(-passed).at[receiver].add(passed)
    labels = jnp.searchsorted(jnp.cumsum(lengths), jnp.arange(rows * top), side="right").astype(jnp.int32)
    grid = labels.reshape(top, rows).T
    grid = grid[jax.random.permutation(jax.random.fold_in(own, 1), rows)]
    offset_by = jax.random.randint(jax.random.fold_in(own, 2), (rows, 1), 0, top)
    return jnp.take_along_axis(grid, (jnp.arange(top)[None, :] + offset_by) % top, axis=1)


def shares(count, total, most, slope, full):
    portions = [(1 << 20) // math.isqrt(grade ** slope) + 1 for grade in range(1, count + 1)]
    largest = most if full else min(most, max(-(-total // count), total * portions[0] // sum(portions)))
    least = 1 if total - largest >= count - 1 else 0
    holding, rest = [largest] + [least] * (count - 1), total - largest - least * (count - 1)
    while rest > 0:
        candidates = [i for i in range(1, count) if holding[i] < largest] or [i for i in range(1, count) if holding[i] < most]
        whole, budget = sum([portions[i] for i in candidates]), rest
        for i in candidates:
            extra = min(most - holding[i], max(1, budget * portions[i] // whole), rest)
            holding[i] = holding[i] + extra
            rest = rest - extra
    return np.array(holding)


def normal_values(key, extent, spread, most, pieces=(), held_as=jnp.bfloat16):
    loudness = shard_levels(key, extent, pieces, -0.22, 0.18) if pieces else 1.0
    result = jax.random.normal(key, extent, jnp.float32) * spread * loudness
    return jnp.minimum(jnp.maximum(result, -most), most).astype(held_as)


def setup_inputs(seed: int = 0) -> dict:
    seeds = jax.random.split(jax.random.key(seed), 7)
    grad_out = normal_values(seeds[0], (TOKENS, D), 1.0, 6.0, ((0, 8),))
    route_ids_keys = jax.random.split(jax.random.fold_in(seeds[1], 1), TOKENS // TOK_DEV)
    route_ids_turns = jax.random.permutation(jax.random.fold_in(seeds[1], 3), TOKENS // TOK_DEV)
    route_ids = jax.vmap(lambda own, number: assign_block(jax.random.fold_in(seeds[1], 2), own, number, TOK_DEV, EXPERTS, TOP, CAP, 2))(route_ids_keys, route_ids_turns).reshape((TOKENS, TOP))
    route_probs = jnp.clip(jnp.exp(math.log(0.5) - 3.224016 * jax.random.uniform(seeds[2], (TOKENS, TOP), jnp.float32) ** shard_levels(seeds[2], (TOKENS, TOP), ((0, 8),), -0.2, 0.2)), 0.019897461, 0.5).astype(jnp.bfloat16)
    gate_act = normal_values(seeds[3], (N_DP, EXPERTS, SLOTS, FF), 1.5, 8.0, ((0, 2), (1, 4), (3, 4)))
    up_act = normal_values(seeds[4], (N_DP, EXPERTS, SLOTS, FF), 1.0, 6.0, ((0, 2), (1, 4), (3, 4)))
    w_down = normal_values(seeds[5], (EXPERTS, FF, D), FF ** -0.5, 0.21875, ((0, 4), (1, 4)))
    return {"grad_out": grad_out, "route_ids": route_ids, "route_probs": route_probs, "gate_act": gate_act, "up_act": up_act, "w_down": w_down}


def expert_backward(inputs, grad_out):
    slot_token, slot_weight, gate_in, up_in, weight = inputs
    valid = slot_token >= 0
    picked = grad_out[jnp.maximum(slot_token, 0)]
    slot_rows = jnp.where(valid[:, :, None], picked, jnp.zeros_like(picked))
    grad_hidden = jnp.einsum("rsd,fd->rsf", slot_rows.astype(jnp.float32), weight.astype(jnp.float32))
    gate_pre = gate_in.astype(jnp.float32)
    up_pre = up_in.astype(jnp.float32)
    sigmoid_gate = jax.nn.sigmoid(gate_pre)
    silu_gate = gate_pre * sigmoid_gate
    hidden = (silu_gate * up_pre).astype(jnp.bfloat16)
    slot_dot = jnp.sum(grad_hidden * hidden.astype(jnp.float32), axis=2)
    grad_scaled = slot_weight[:, :, None] * grad_hidden
    grad_up = (grad_scaled * silu_gate).astype(jnp.bfloat16)
    grad_gate = (grad_scaled * up_pre * sigmoid_gate * (1.0 + gate_pre * (1.0 - sigmoid_gate))).astype(jnp.bfloat16)
    scaled_rows = (slot_weight[:, :, None] * slot_rows.astype(jnp.float32)).astype(jnp.bfloat16)
    replica_grad = jnp.einsum("rsf,rsd->rfd", hidden.astype(jnp.float32), scaled_rows.astype(jnp.float32))
    rounded = lax.optimization_barrier(replica_grad.astype(jnp.bfloat16))
    grad_weight = jnp.sum(rounded.astype(jnp.float32), axis=0).astype(jnp.bfloat16)
    return grad_gate, grad_up, grad_weight, slot_dot


def reference(grad_out, route_ids, route_probs, gate_act, up_act, w_down):
    block_count = N_EXPERT * N_DP
    route_count = TOK_DEV * TOP
    routes_block = route_ids.reshape(block_count, route_count).astype(jnp.int32)
    matches = (routes_block[:, :, None] == jnp.arange(EXPERTS, dtype=jnp.int32)[None, None, :]).astype(jnp.int32)
    earlier = jnp.cumsum(matches, axis=1) - matches
    position = jnp.sum(earlier * matches, axis=2).astype(jnp.int32)
    block_index = jnp.arange(block_count, dtype=jnp.int32)[:, None]
    source = block_index // N_DP
    replica = jnp.broadcast_to(block_index % N_DP, (block_count, route_count))
    slot = (source * CAP + position).astype(jnp.int32)
    token_index = (block_index * TOK_DEV + jnp.arange(route_count, dtype=jnp.int32)[None, :] // TOP).astype(jnp.int32)
    flat_replica = replica.reshape(-1)
    flat_expert = routes_block.reshape(-1)
    flat_slot = slot.reshape(-1)
    slot_token = jnp.full((N_DP, EXPERTS, SLOTS), -1, jnp.int32).at[flat_replica, flat_expert, flat_slot].set(token_index.reshape(-1))
    slot_weight = jnp.zeros((N_DP, EXPERTS, SLOTS), jnp.float32).at[flat_replica, flat_expert, flat_slot].set(route_probs.reshape(-1).astype(jnp.float32))
    inputs = (jnp.transpose(slot_token, (1, 0, 2)), jnp.transpose(slot_weight, (1, 0, 2)),
              jnp.transpose(gate_act, (1, 0, 2, 3)), jnp.transpose(up_act, (1, 0, 2, 3)), w_down)
    grad_gate, grad_up, grad_w_down, slot_dot = lax.map(lambda item: expert_backward(item, grad_out), inputs)
    grad_gate = jnp.transpose(grad_gate, (1, 0, 2, 3))
    grad_up = jnp.transpose(grad_up, (1, 0, 2, 3))
    slot_dot = jnp.transpose(slot_dot, (1, 0, 2))
    grad_probs = slot_dot[flat_replica, flat_expert, flat_slot].reshape(TOKENS, TOP)
    return (grad_gate, grad_up, grad_w_down, grad_probs)
```

```python
import functools
import jax
import jax.numpy as jnp
from jax import lax
from jax.experimental import pallas as pl
from jax.experimental.pallas import tpu as pltpu
from jax.sharding import PartitionSpec as P


def on_device_wide(grad_out, route_ids, route_probs, gate_act, up_act, w_down):
    tok_count = grad_out.shape[0]
    top_count = route_ids.shape[1]
    expert_count = lax.axis_size("expert")
    tensor_count = lax.axis_size("tensor")
    local_experts = w_down.shape[0]
    experts = local_experts * expert_count
    slot_count = gate_act.shape[2]
    capacity = slot_count // expert_count
    model_width = grad_out.shape[1]
    quarter = model_width // tensor_count
    route_flat = route_ids.reshape(-1)
    expert_iota = lax.broadcasted_iota(jnp.int32, (1, experts), 1)
    matches = (route_flat[:, None] == expert_iota).astype(jnp.int32)
    earlier = jnp.cumsum(matches, axis=0) - matches
    position = jnp.sum(earlier * matches, axis=1)
    target = route_flat * capacity + position
    cell_iota = lax.broadcasted_iota(jnp.int32, (1, experts * capacity), 1)
    chosen = target[:, None] == cell_iota
    chosen_weight = chosen.astype(jnp.float32)
    token_chosen = jnp.sum(
        chosen_weight.reshape(tok_count, top_count, experts * capacity), axis=1
    ).astype(jnp.bfloat16)
    own_columns = lax.dynamic_slice_in_dim(grad_out, lax.axis_index("tensor") * quarter, quarter, 1)
    send_rows = jnp.einsum(
        "nf,nd->fd", token_chosen, own_columns, preferred_element_type=jnp.float32
    ).astype(jnp.bfloat16)
    send_probs = jnp.sum(
        chosen_weight * route_probs.reshape(-1).astype(jnp.float32)[:, None], axis=0
    ).astype(jnp.bfloat16)
    send_rows = send_rows.reshape(expert_count, local_experts, capacity, quarter)
    send_probs = send_probs.reshape(expert_count, local_experts, capacity)
    arrived_rows, arrived_probs = (
        lax.all_to_all(send_rows, "expert", split_axis=0, concat_axis=0, tiled=True),
        lax.all_to_all(send_probs, "expert", split_axis=0, concat_axis=0, tiled=True),
    )
    gathered = lax.all_gather(arrived_rows, "tensor", axis=3, tiled=True)
    slot_rows = jnp.transpose(gathered, (1, 0, 2, 3)).reshape(
        local_experts, slot_count, model_width
    )
    slot_probs = (
        jnp.transpose(arrived_probs, (1, 0, 2))
        .reshape(local_experts, slot_count)
        .astype(jnp.float32)
    )
    gate_pre = gate_act[0].astype(jnp.float32)
    up_pre = up_act[0].astype(jnp.float32)
    grad_hidden = jnp.einsum("jsd,jfd->jsf", slot_rows, w_down, preferred_element_type=jnp.float32)
    sigmoid_gate = jax.nn.sigmoid(gate_pre)
    silu_gate = gate_pre * sigmoid_gate
    hidden = (silu_gate * up_pre).astype(jnp.bfloat16)
    partial_dot = jnp.sum(grad_hidden * hidden.astype(jnp.float32), axis=2)
    grad_scaled = slot_probs[:, :, None] * grad_hidden
    grad_up = (grad_scaled * silu_gate).astype(jnp.bfloat16)
    grad_gate = (
        grad_scaled * up_pre * sigmoid_gate * (1.0 + gate_pre * (1.0 - sigmoid_gate))
    ).astype(jnp.bfloat16)
    scaled_rows = (slot_probs[:, :, None] * slot_rows.astype(jnp.float32)).astype(jnp.bfloat16)
    replica_count = lax.axis_size("dp")
    column_count = model_width // replica_count
    split_rows = jnp.transpose(
        scaled_rows.reshape(local_experts, slot_count, replica_count, column_count), (2, 0, 1, 3)
    )
    columns = lax.all_to_all(split_rows, "dp", split_axis=0, concat_axis=0, tiled=True)
    initial = jnp.zeros((local_experts, hidden.shape[2], column_count), jnp.float32)
    hidden_block = lax.all_gather(hidden[None], "dp", axis=0, tiled=True)

    def add_member(member, summed):
        hid_one = lax.dynamic_index_in_dim(hidden_block, member, 0, keepdims=False)
        col_one = lax.dynamic_index_in_dim(columns, member, 0, keepdims=False)
        term = jnp.einsum("jsf,jsd->jfd", hid_one, col_one, preferred_element_type=jnp.float32)
        rounded = lax.optimization_barrier(term.astype(jnp.bfloat16))
        return summed + rounded.astype(jnp.float32)

    grad_weight = lax.fori_loop(0, hidden_block.shape[0], add_member, initial).astype(jnp.bfloat16)
    prob_cells = jnp.transpose(
        partial_dot.reshape(local_experts, expert_count, capacity), (1, 0, 2)
    )
    prob_cells = lax.psum(prob_cells, "tensor")
    returned = lax.all_to_all(prob_cells, "expert", split_axis=0, concat_axis=0, tiled=True)
    returned_flat = returned.reshape(-1)
    grad_probs = jnp.sum(jnp.where(chosen, returned_flat[None, :], 0.0), axis=1).reshape(
        tok_count, top_count
    )
    return (grad_gate[None], grad_up[None], grad_weight, grad_probs)


MESH = pl.DeviceIdType.MESH
RING = 6


def gather_kernel(
    sizes, cap, x_ref, ids_ref, probs_ref, gate_ref, up_ref, w_ref,
    rows_out, hs_out, gh_out, prob_out, back,
    tok, oth, ids, probs, gate, up, wbuf, rows, far_rows, one, acc, gh, hid, hs, hs_far, prob, cells,
    lx, lm, la, lw, lo, zs, zr, ms, mr, ys, yr, as_, ar, bs, br, xs, xr, ps, pr, qs, qr, us, ur, hsem, rs, rr,
):
    tn, en, rn = sizes
    f32, bf16 = jnp.float32, jnp.bfloat16
    t, e, d = lax.axis_index("tensor"), lax.axis_index("expert"), lax.axis_index("dp")
    plane, core = t // 2, lax.rem(t, 2)
    across = lax.rem(t + 2, tn)
    mate = t + 1 - 2 * core
    far = 1 - d
    steps = tok.shape[0] // 2
    per = steps // 2
    tokens, width = x_ref.shape
    region = tok.shape[2]
    piece = region // 2
    local, slots, units = gh.shape
    total = en * tokens

    def block(k):
        return lax.rem(e - k + en, en)

    def index(s, p):
        half = jnp.where(s < per, far, d)
        return half * steps + p * per + lax.rem(s, per)

    def part(buf, g, b, q):
        return buf.at[g, pl.ds(pl.multiple_of(b * tokens, tokens), tokens), pl.ds(pl.multiple_of(q * piece, piece), piece)]

    def wide_part(buf, g, q):
        return buf.at[g, :, pl.ds(pl.multiple_of(q * piece, piece), piece)]

    def remote(src, dst, ssem, rsem, peer):
        return pltpu.make_async_remote_copy(
            src_ref=src, dst_ref=dst, send_sem=ssem, recv_sem=rsem, device_id=peer, device_id_type=MESH
        )

    def along(s, k):
        ref = part(tok, index(s, plane), e, core)
        return remote(ref, ref, zs.at[s, k - 1], zr.at[s, k - 1], (t, lax.rem(e + k, en), d))

    def over(s, k):
        ref = part(tok, index(s, plane), block(k), core)
        return remote(ref, ref, ys.at[s, k - 1], yr.at[s, k - 1], (across, e, d))

    def mate_own(s, k):
        ref = part(tok, index(s, plane), block(k), core)
        return remote(ref, ref, as_.at[s, k - 1], ar.at[s, k - 1], (mate, e, d))

    def mate_over(s, k):
        ref = part(tok, index(s, 1 - plane), block(k), core)
        return remote(ref, ref, bs.at[s, k - 1], br.at[s, k - 1], (mate, e, d))

    def far_send(i):
        return remote(
            wide_part(tok, index(i, plane), core), wide_part(oth, plane * per + i, core), xs.at[i], xr.at[i], (t, e, far)
        )

    def far_over(i):
        ref = wide_part(oth, plane * per + i, core)
        return remote(ref, ref, ps.at[i], pr.at[i], (across, e, d))

    def far_mate(i):
        ref = wide_part(oth, plane * per + i, core)
        return remote(ref, ref, qs.at[i], qr.at[i], (mate, e, d))

    def far_mate_over(i):
        ref = wide_part(oth, (1 - plane) * per + i, core)
        return remote(ref, ref, us.at[i], ur.at[i], (mate, e, d))

    def hid_send():
        return remote(hs, hs_far, hsem.at[0], hsem.at[1], (t, e, far))

    def weights(r):
        g = index(r // 2, jnp.where(lax.rem(r, 2) == 0, plane, 1 - plane))
        slot = lax.rem(r, RING)
        return pltpu.make_async_copy(
            w_ref.at[:, :, pl.ds(pl.multiple_of(g * region, region), region)], wbuf.at[slot], lw.at[slot]
        )

    def load_own(g):
        return pltpu.make_async_copy(
            x_ref.at[:, pl.ds(g * region, region)],
            tok.at[g, pl.ds(pl.multiple_of(e * tokens, tokens), tokens), :], lx.at[g],
        )

    loads = [load_own(g) for g in range(2 * steps)]
    metas = [
        pltpu.make_async_copy(ids_ref, ids.at[e, d], lm.at[0]),
        pltpu.make_async_copy(probs_ref, probs.at[e, d], lm.at[1]),
    ]
    acts = [pltpu.make_async_copy(gate_ref.at[0], gate, la.at[0]), pltpu.make_async_copy(up_ref.at[0], up, la.at[1])]
    for copy in metas + loads + acts:
        copy.start()
    for r in range(RING):
        weights(r).start()

    others = []
    for i in range(en):
        for j in range(rn):
            if i or j:
                others.append((t, lax.rem(e + i, en), lax.rem(d + j, rn)))
    group = []
    for i in range(tn):
        for j in range(en):
            if i or j:
                group.append((lax.rem(t + i, tn), lax.rem(e + j, en), d))
    greet = group + [peer for n, peer in enumerate(others) if (n + 1) % rn]
    barrier = pltpu.get_barrier_semaphore()
    for peer in greet:
        pl.semaphore_signal(barrier, inc=1, device_id=peer, device_id_type=MESH)
    pl.semaphore_wait(barrier, len(greet))

    for copy in metas + loads:
        copy.wait()
    for s in range(steps):
        for k in range(1, en):
            along(s, k).start()
    sent = []
    for i, peer in enumerate(others):
        sent.append(remote(ids_ref, ids.at[e, d], ms.at[0, i], mr.at[0, i], peer))
        sent.append(remote(probs_ref, probs.at[e, d], ms.at[1, i], mr.at[1, i], peer))
    for copy in sent:
        copy.start()

    for copy in acts:
        copy.wait()

    def prepare(j, carry):
        g = gate[j].astype(f32)
        hid[j] = (g * jax.nn.sigmoid(g) * up[j].astype(f32)).astype(bf16)
        acc[j] = jnp.zeros(acc.shape[1:], f32)
        return carry

    lax.fori_loop(0, local, prepare, 0)

    def pass_on(s):
        for k in range(1, en):
            along(s, k).wait_recv()
            over(s, k).start()
            mate_own(s, k).start()

    pass_on(0)
    far_send(0).start()
    for copy in sent:
        copy.wait_recv()

    spot = lax.broadcasted_iota(jnp.int32, (total, total), 0)
    lane = lax.broadcasted_iota(jnp.int32, (total, total), 1)
    below = ((spot < lane) & (spot // tokens == lane // tokens)).astype(f32).astype(bf16)
    here = e * local + lax.broadcasted_iota(jnp.int32, (local, total), 0)
    origin = (lax.broadcasted_iota(jnp.int32, (local, total), 1) // tokens * cap).astype(f32)
    top = ids.shape[2]

    def find(which, replica):
        named = jnp.zeros((local, total), f32)
        carried = jnp.zeros((local, total), f32)
        id_all = jnp.concatenate([ids[b, replica] for b in range(en)], axis=1)
        pr_all = jnp.concatenate([probs[b, replica].astype(f32) for b in range(en)], axis=1)
        for k in range(top):
            hit = id_all[k : k + 1, :] == here
            named = jnp.where(hit, 1.0, named)
            carried = jnp.where(hit, pr_all[k : k + 1, :], carried)
        position = jnp.dot(named.astype(bf16), below, preferred_element_type=f32)
        code = jnp.where(named > 0.0, position + origin, -1.0)
        match = code[:, None, :] == lax.broadcasted_iota(jnp.int32, (local, slots, total), 1).astype(f32)
        one[which] = jnp.where(match, 1.0, 0.0).reshape(local * slots, total).astype(bf16)
        return jnp.sum(jnp.where(match, carried[:, None, :], 0.0), axis=2, keepdims=True)

    prob[...] = find(0, d)
    find(1, far)
    hs[...] = (prob[...] * hid[...].astype(f32)).astype(bf16)

    def pick(which, src):
        found = jnp.dot(one[which], src, preferred_element_type=f32)
        return found.reshape(local, slots, region).astype(bf16)

    def store_rows(s, p):
        g = index(s, p) - d * steps
        return pltpu.make_async_copy(
            rows.at[s - per, p],
            rows_out.at[:, pl.ds(0, slots), pl.ds(pl.multiple_of(g * region, region), region)],
            lo.at[s - per, p],
        )

    def work(s, r, p, mid):
        weights(r).wait()
        g = index(s, p)
        into = rows.at[lax.rem(s, per), p]
        into[...] = pick(0, tok[g])

        @pl.when(s >= per)
        def _():
            store_rows(s, p).start()

        slot = lax.rem(r, RING)

        def one_expert(j, carry):
            acc[j] += lax.dot_general(
                wbuf[slot, j], into[j], (((1,), (1,)), ((), ())), preferred_element_type=f32
            )
            return carry

        lax.fori_loop(0, local // 2, one_expert, 0, unroll=4)
        mid()
        lax.fori_loop(local // 2, local, one_expert, 0, unroll=4)

        @pl.when(r + RING < 2 * steps)
        def _():
            weights(r + RING).start()

    def step(s, carry):
        for k in range(1, en):
            mate_own(s, k).wait_recv()

        def middle():
            for k in range(1, en):
                over(s, k).wait_recv()
                mate_over(s, k).start()

            @pl.when(s + 1 < steps)
            def _():
                pass_on(s + 1)

            @pl.when(s + 1 < per)
            def _():
                far_send(s + 1).start()

            @pl.when(s + 1 == per)
            def _():
                hid_send().start()

        work(s, 2 * s, plane, middle)
        for k in range(1, en):
            mate_over(s, k).wait_recv()

        def later():
            @pl.when(s >= per)
            def _():
                i = s - per
                far_send(i).wait_recv()
                far_over(i).start()
                far_mate(i).start()

        work(s, 2 * s + 1, 1 - plane, later)
        return carry

    lax.fori_loop(0, steps, step, 0)

    column = lax.broadcasted_iota(jnp.int32, (slots, cells.shape[2]), 1)

    def finish(j, dots):
        grad = acc[j].T
        gh[j] = grad
        dot = jnp.sum(grad * hid[j].astype(f32), axis=1, keepdims=True)
        return jnp.where(column == j, dot, dots)

    dots = lax.fori_loop(0, local, finish, jnp.zeros(column.shape, f32), unroll=4)
    for b in range(en):
        cells[b, pl.ds(0, cap), :] = dots[b * cap : (b + 1) * cap, :]
        cells[b, pl.ds(cap, cells.shape[1] - cap), :] = jnp.zeros((cells.shape[1] - cap, cells.shape[2]), f32)
    for i in range(per):
        far_over(i).wait_recv()
        far_mate_over(i).start()
    returns = [
        remote(cells.at[peer[1]], back.at[t, e], rs.at[i], rr.at[i], peer) for i, peer in enumerate(group)
    ]
    for copy in returns:
        copy.start()
    back[t, e] = cells[e]
    outs = [
        pltpu.make_async_copy(gh, gh_out, lm.at[0]),
        pltpu.make_async_copy(prob, prob_out, lm.at[1]),
        pltpu.make_async_copy(hs, hs_out.at[:, pl.ds(0, slots), :], la.at[0]),
    ]
    for copy in outs:
        copy.start()
    for i in range(per):
        far_mate(i).wait_recv()
        far_mate_over(i).wait_recv()
    far_outs = []
    for q in range(steps):
        far_rows[q] = pick(1, oth[q])
        copy = pltpu.make_async_copy(
            far_rows.at[q], rows_out.at[:, pl.ds(slots, slots), pl.ds(q * region, region)], lx.at[q]
        )
        copy.start()
        far_outs.append(copy)
    hid_send().wait_recv()
    copy = pltpu.make_async_copy(hs_far, hs_out.at[:, pl.ds(slots, slots), :], la.at[1])
    copy.start()
    outs.append(copy)

    def drain(s, carry):
        for k in range(1, en):
            along(s, k).wait_send()
            over(s, k).wait_send()
            mate_own(s, k).wait_send()
            mate_over(s, k).wait_send()
        return carry

    lax.fori_loop(0, steps, drain, 0)
    for copy in sent:
        copy.wait_send()
    hid_send().wait_send()
    for i in range(per):
        far_send(i).wait_send()
        far_over(i).wait_send()
        far_mate(i).wait_send()
        far_mate_over(i).wait_send()
        for p in range(2):
            store_rows(per + i, p).wait()
    for copy in returns:
        copy.wait()
    for copy in outs + far_outs:
        copy.wait()


def expert_kernel(cap, local, rows, hs, gh, gate, up, prob, back, ids, grad_gate, grad_up, grad_w, grad_probs):
    f32, bf16 = jnp.float32, jnp.bfloat16
    for k in range(rows.shape[0]):
        turned = hs[k].astype(f32).T.astype(bf16)
        grad_w[k] = jnp.dot(turned, rows[k], preferred_element_type=f32).astype(bf16)
        g = gate[0, k].astype(f32)
        u = up[0, k].astype(f32)
        s = jax.nn.sigmoid(g)
        weighted = prob[k] * gh[k]
        grad_up[0, k] = (weighted * (g * s)).astype(bf16)
        grad_gate[0, k] = (weighted * u * s * (1.0 + g * (1.0 - s))).astype(bf16)

    @pl.when(pl.program_id(0) == 0)
    def _():
        top, tokens = ids.shape
        tn, en = back.shape[0], back.shape[1]
        summed = back[0]
        for i in range(1, tn):
            summed = summed + back[i]
        cell = jnp.concatenate([summed[b].T[:local] for b in range(en)], axis=0)
        every = lax.broadcasted_iota(jnp.int32, (en * local, tokens), 0)
        spot = lax.broadcasted_iota(jnp.int32, (tokens, tokens), 0)
        lane = lax.broadcasted_iota(jnp.int32, (tokens, tokens), 1)
        below = (spot < lane).astype(f32).astype(bf16)
        named = jnp.zeros(every.shape, f32)
        for k in range(top):
            named = jnp.where(ids[k : k + 1, :] == every, 1.0, named)
        before = jnp.dot(named.astype(bf16), below, preferred_element_type=f32)
        value = jnp.zeros(every.shape, f32)
        for p in range(cap):
            value = jnp.where(before == float(p), cell[:, p : p + 1], value)
        for k in range(top):
            found = jnp.where(ids[k : k + 1, :] == every, value, 0.0)
            grad_probs[k : k + 1, :] = jnp.sum(found, axis=0, keepdims=True)


def on_device(grad_out, route_ids, route_probs, gate_act, up_act, w_down):
    tokens, width = grad_out.shape
    top = route_ids.shape[1]
    tn, en, rn = lax.axis_size("tensor"), lax.axis_size("expert"), lax.axis_size("dp")
    local, units, slots = w_down.shape[0], w_down.shape[1], gate_act.shape[2]
    cap = slots // en
    half = width // rn
    steps = 4
    per = steps // 2
    region = width // (2 * steps)
    total = en * tokens
    f32, bf16 = jnp.float32, jnp.bfloat16
    sem = pltpu.SemaphoreType.DMA
    anyspace = pl.BlockSpec(memory_space=pl.ANY)
    vmem = pl.BlockSpec(memory_space=pltpu.VMEM)
    ids_turned = route_ids.T
    both = rn * slots
    hidden_shape = (local, slots, units)
    rows, hs, gh, prob, back = pl.pallas_call(
        functools.partial(gather_kernel, (tn, en, rn), cap),
        out_shape=(
            jax.ShapeDtypeStruct((local, both, half), bf16),
            jax.ShapeDtypeStruct((local, both, units), bf16),
            jax.ShapeDtypeStruct(hidden_shape, f32),
            jax.ShapeDtypeStruct((local, slots, 1), f32),
            jax.ShapeDtypeStruct((tn, en, 8, 128), f32),
        ),
        in_specs=[anyspace, vmem, vmem, anyspace, anyspace, anyspace],
        out_specs=(anyspace, anyspace, anyspace, anyspace, vmem),
        scratch_shapes=[
            pltpu.VMEM((2 * steps, total, region), bf16),
            pltpu.VMEM((steps, total, region), bf16),
            pltpu.VMEM((en, rn, top, tokens), jnp.int32),
            pltpu.VMEM((en, rn, top, tokens), bf16),
            pltpu.VMEM(hidden_shape, bf16),
            pltpu.VMEM(hidden_shape, bf16),
            pltpu.VMEM((RING, local, units, region), bf16),
            pltpu.VMEM((per, 2, local, slots, region), bf16),
            pltpu.VMEM((steps, local, slots, region), bf16),
            pltpu.VMEM((rn, local * slots, total), bf16),
            pltpu.VMEM((local, units, slots), f32),
            pltpu.VMEM(hidden_shape, f32),
            pltpu.VMEM(hidden_shape, bf16),
            pltpu.VMEM(hidden_shape, bf16),
            pltpu.VMEM(hidden_shape, bf16),
            pltpu.VMEM((local, slots, 1), f32),
            pltpu.VMEM((en, 8, 128), f32),
            sem((2 * steps,)), sem((2,)), sem((2,)), sem((RING,)), sem((per, 2)),
            sem((steps, en - 1)), sem((steps, en - 1)),
            sem((2, en * rn - 1)), sem((2, en * rn - 1)),
            sem((steps, en - 1)), sem((steps, en - 1)),
            sem((steps, en - 1)), sem((steps, en - 1)),
            sem((steps, en - 1)), sem((steps, en - 1)),
            sem((per,)), sem((per,)), sem((per,)), sem((per,)), sem((per,)), sem((per,)), sem((per,)), sem((per,)),
            sem((2,)), sem((tn * en - 1,)), sem((tn * en - 1,)),
        ],
        compiler_params=pltpu.CompilerParams(
            collective_id=0, has_side_effects=True, vmem_limit_bytes=67043328
        ),
    )(grad_out, ids_turned, route_probs.T, gate_act, up_act, w_down)

    batch = 2

    def block(*shape):
        return pl.BlockSpec((batch,) + shape, lambda i: (i,) + (0,) * len(shape))

    act = pl.BlockSpec((1, batch, slots, units), lambda i: (0, i, 0, 0))
    act_shape = jax.ShapeDtypeStruct((1, local, slots, units), bf16)
    grad_gate, grad_up, grad_w, grad_probs = pl.pallas_call(
        functools.partial(expert_kernel, cap, local),
        grid=(local // batch,),
        in_specs=[
            block(both, half), block(both, units), block(slots, units), act, act, block(slots, 1), vmem, vmem,
        ],
        out_specs=(act, act, block(units, half), vmem),
        out_shape=(
            act_shape, act_shape,
            jax.ShapeDtypeStruct((local, units, half), bf16),
            jax.ShapeDtypeStruct((top, tokens), f32),
        ),
    )(rows, hs, gh, gate_act, up_act, prob, back, ids_turned)
    return grad_gate, grad_up, grad_w, grad_probs.T


def solution(mesh):
    sizes = mesh.shape
    small = sizes["tensor"] == 4 and sizes["dp"] == 2 and sizes["expert"] <= 8
    placed = (
        P(("expert", "dp"), None),
        P(("expert", "dp"), None),
        P(("expert", "dp"), None),
        P("dp", "expert", None, "tensor"),
        P("dp", "expert", None, "tensor"),
        P("expert", "tensor", None),
    )
    return jax.shard_map(
        on_device if small else on_device_wide,
        mesh=mesh,
        in_specs=placed,
        out_specs=(
            P("dp", "expert", None, "tensor"),
            P("dp", "expert", None, "tensor"),
            P("expert", "tensor", "dp"),
            P(("expert", "dp"), None),
        ),
        check_vma=False,
    )
```

```python
import functools
import jax
import jax.numpy as jnp
from jax import lax
from jax.experimental import pallas as pl
from jax.experimental.pallas import tpu as pltpu
from jax.sharding import PartitionSpec as P


def on_device_wide(grad_out, route_ids, route_probs, gate_act, up_act, w_down):
    tok_count = grad_out.shape[0]
    top_count = route_ids.shape[1]
    expert_count = lax.axis_size("expert")
    tensor_count = lax.axis_size("tensor")
    local_experts = w_down.shape[0]
    experts = local_experts * expert_count
    slot_count = gate_act.shape[2]
    capacity = slot_count // expert_count
    model_width = grad_out.shape[1]
    quarter = model_width // tensor_count
    route_flat = route_ids.reshape(-1)
    expert_iota = lax.broadcasted_iota(jnp.int32, (1, experts), 1)
    matches = (route_flat[:, None] == expert_iota).astype(jnp.int32)
    earlier = jnp.cumsum(matches, axis=0) - matches
    position = jnp.sum(earlier * matches, axis=1)
    target = route_flat * capacity + position
    cell_iota = lax.broadcasted_iota(jnp.int32, (1, experts * capacity), 1)
    chosen = target[:, None] == cell_iota
    chosen_weight = chosen.astype(jnp.float32)
    token_chosen = jnp.sum(
        chosen_weight.reshape(tok_count, top_count, experts * capacity), axis=1
    ).astype(jnp.bfloat16)
    own_columns = lax.dynamic_slice_in_dim(grad_out, lax.axis_index("tensor") * quarter, quarter, 1)
    send_rows = jnp.einsum(
        "nf,nd->fd", token_chosen, own_columns, preferred_element_type=jnp.float32
    ).astype(jnp.bfloat16)
    send_probs = jnp.sum(
        chosen_weight * route_probs.reshape(-1).astype(jnp.float32)[:, None], axis=0
    ).astype(jnp.bfloat16)
    send_rows = send_rows.reshape(expert_count, local_experts, capacity, quarter)
    send_probs = send_probs.reshape(expert_count, local_experts, capacity)
    arrived_rows, arrived_probs = (
        lax.all_to_all(send_rows, "expert", split_axis=0, concat_axis=0, tiled=True),
        lax.all_to_all(send_probs, "expert", split_axis=0, concat_axis=0, tiled=True),
    )
    gathered = lax.all_gather(arrived_rows, "tensor", axis=3, tiled=True)
    slot_rows = jnp.transpose(gathered, (1, 0, 2, 3)).reshape(
        local_experts, slot_count, model_width
    )
    slot_probs = (
        jnp.transpose(arrived_probs, (1, 0, 2))
        .reshape(local_experts, slot_count)
        .astype(jnp.float32)
    )
    gate_pre = gate_act[0].astype(jnp.float32)
    up_pre = up_act[0].astype(jnp.float32)
    grad_hidden = jnp.einsum("jsd,jfd->jsf", slot_rows, w_down, preferred_element_type=jnp.float32)
    sigmoid_gate = jax.nn.sigmoid(gate_pre)
    silu_gate = gate_pre * sigmoid_gate
    hidden = (silu_gate * up_pre).astype(jnp.bfloat16)
    partial_dot = jnp.sum(grad_hidden * hidden.astype(jnp.float32), axis=2)
    grad_scaled = slot_probs[:, :, None] * grad_hidden
    grad_up = (grad_scaled * silu_gate).astype(jnp.bfloat16)
    grad_gate = (
        grad_scaled * up_pre * sigmoid_gate * (1.0 + gate_pre * (1.0 - sigmoid_gate))
    ).astype(jnp.bfloat16)
    scaled_rows = (slot_probs[:, :, None] * slot_rows.astype(jnp.float32)).astype(jnp.bfloat16)
    replica_count = lax.axis_size("dp")
    column_count = model_width // replica_count
    split_rows = jnp.transpose(
        scaled_rows.reshape(local_experts, slot_count, replica_count, column_count), (2, 0, 1, 3)
    )
    columns = lax.all_to_all(split_rows, "dp", split_axis=0, concat_axis=0, tiled=True)
    initial = jnp.zeros((local_experts, hidden.shape[2], column_count), jnp.float32)
    hidden_block = lax.all_gather(hidden[None], "dp", axis=0, tiled=True)

    def add_member(member, summed):
        hid_one = lax.dynamic_index_in_dim(hidden_block, member, 0, keepdims=False)
        col_one = lax.dynamic_index_in_dim(columns, member, 0, keepdims=False)
        term = jnp.einsum("jsf,jsd->jfd", hid_one, col_one, preferred_element_type=jnp.float32)
        rounded = lax.optimization_barrier(term.astype(jnp.bfloat16))
        return summed + rounded.astype(jnp.float32)

    grad_weight = lax.fori_loop(0, hidden_block.shape[0], add_member, initial).astype(jnp.bfloat16)
    prob_cells = jnp.transpose(
        partial_dot.reshape(local_experts, expert_count, capacity), (1, 0, 2)
    )
    prob_cells = lax.psum(prob_cells, "tensor")
    returned = lax.all_to_all(prob_cells, "expert", split_axis=0, concat_axis=0, tiled=True)
    returned_flat = returned.reshape(-1)
    grad_probs = jnp.sum(jnp.where(chosen, returned_flat[None, :], 0.0), axis=1).reshape(
        tok_count, top_count
    )
    return (grad_gate[None], grad_up[None], grad_weight, grad_probs)


MESH = pl.DeviceIdType.MESH
RING = 6


def gather_kernel(
    sizes, cap, x_ref, ids_ref, probs_ref, gate_ref, up_ref, w_ref,
    rows_out, hs_out, gate_out, up_out, back,
    tok, oth, ids, probs, gate, up, wbuf, rows, far_rows, one, acc, flat, gh, hid, hs, hs_far, grad_gate, grad_up, prob, cells,
    lx, lm, la, lw, lo, zs, zr, ms, mr, ys, yr, as_, ar, bs, br, xs, xr, ps, pr, qs, qr, us, ur, hsem, rs, rr,
):
    tn, en, rn = sizes
    f32, bf16 = jnp.float32, jnp.bfloat16
    t, e, d = lax.axis_index("tensor"), lax.axis_index("expert"), lax.axis_index("dp")
    plane, core = t // 2, lax.rem(t, 2)
    across = lax.rem(t + 2, tn)
    mate = t + 1 - 2 * core
    far = 1 - d
    steps = tok.shape[0] // 2
    per = steps // 2
    tokens, width = x_ref.shape
    region = tok.shape[2]
    piece = region // 2
    local, slots, units = gh.shape
    total = en * tokens

    def block(k):
        return lax.rem(e - k + en, en)

    def index(s, p):
        half = jnp.where(s < per, far, d)
        return half * steps + p * per + lax.rem(s, per)

    def part(buf, g, b, q):
        return buf.at[g, pl.ds(pl.multiple_of(b * tokens, tokens), tokens), pl.ds(pl.multiple_of(q * piece, piece), piece)]

    def wide_part(buf, g, q):
        return buf.at[g, :, pl.ds(pl.multiple_of(q * piece, piece), piece)]

    def remote(src, dst, ssem, rsem, peer):
        return pltpu.make_async_remote_copy(
            src_ref=src, dst_ref=dst, send_sem=ssem, recv_sem=rsem, device_id=peer, device_id_type=MESH
        )

    def along(s, k):
        ref = part(tok, index(s, plane), e, core)
        return remote(ref, ref, zs.at[s, k - 1], zr.at[s, k - 1], (t, lax.rem(e + k, en), d))

    def over(s, k):
        ref = part(tok, index(s, plane), block(k), core)
        return remote(ref, ref, ys.at[s, k - 1], yr.at[s, k - 1], (across, e, d))

    def mate_own(s, k):
        ref = part(tok, index(s, plane), block(k), core)
        return remote(ref, ref, as_.at[s, k - 1], ar.at[s, k - 1], (mate, e, d))

    def mate_over(s, k):
        ref = part(tok, index(s, 1 - plane), block(k), core)
        return remote(ref, ref, bs.at[s, k - 1], br.at[s, k - 1], (mate, e, d))

    def far_send(i):
        return remote(
            wide_part(tok, index(i, plane), core), wide_part(oth, plane * per + i, core), xs.at[i], xr.at[i], (t, e, far)
        )

    def far_over(i):
        ref = wide_part(oth, plane * per + i, core)
        return remote(ref, ref, ps.at[i], pr.at[i], (across, e, d))

    def far_mate(i):
        ref = wide_part(oth, plane * per + i, core)
        return remote(ref, ref, qs.at[i], qr.at[i], (mate, e, d))

    def far_mate_over(i):
        ref = wide_part(oth, (1 - plane) * per + i, core)
        return remote(ref, ref, us.at[i], ur.at[i], (mate, e, d))

    def hid_send():
        return remote(hs, hs_far, hsem.at[0], hsem.at[1], (t, e, far))

    def turn(r):
        own = (r == 0) | ((lax.rem(r, 2) == 1) & (r < 2 * steps - 1))
        s = jnp.where(r == 0, 0, jnp.where(own, (r + 1) // 2, jnp.where(r == 2 * steps - 1, steps - 1, r // 2 - 1)))
        return s, own

    def weights(r):
        s, own = turn(r)
        g = index(s, jnp.where(own, plane, 1 - plane))
        slot = lax.rem(r, RING)
        return pltpu.make_async_copy(
            w_ref.at[:, :, pl.ds(pl.multiple_of(g * region, region), region)], wbuf.at[slot], lw.at[slot]
        )

    def load_own(g):
        return pltpu.make_async_copy(
            x_ref.at[:, pl.ds(g * region, region)],
            tok.at[g, pl.ds(pl.multiple_of(e * tokens, tokens), tokens), :], lx.at[g],
        )

    loads = [load_own(g) for g in range(2 * steps)]
    metas = [
        pltpu.make_async_copy(ids_ref, ids.at[e, d], lm.at[0]),
        pltpu.make_async_copy(probs_ref, probs.at[e, d], lm.at[1]),
    ]
    acts = [pltpu.make_async_copy(gate_ref.at[0], gate, la.at[0]), pltpu.make_async_copy(up_ref.at[0], up, la.at[1])]
    for copy in metas + loads + acts:
        copy.start()

    others = []
    for i in range(en):
        for j in range(rn):
            if i or j:
                others.append((t, lax.rem(e + i, en), lax.rem(d + j, rn)))
    group = []
    for i in range(tn):
        for j in range(en):
            if i or j:
                group.append((lax.rem(t + i, tn), lax.rem(e + j, en), d))
    greet = group + [peer for n, peer in enumerate(others) if (n + 1) % rn]
    barrier = pltpu.get_barrier_semaphore()
    for peer in greet:
        pl.semaphore_signal(barrier, inc=1, device_id=peer, device_id_type=MESH)
    for copy in metas + loads:
        copy.wait()
    for r in range(RING):
        weights(r).start()
    pl.semaphore_wait(barrier, len(greet))

    sent = []
    for i, peer in enumerate(others):
        sent.append(remote(ids.at[e, d], ids.at[e, d], ms.at[0, i], mr.at[0, i], peer))
        sent.append(remote(probs.at[e, d], probs.at[e, d], ms.at[1, i], mr.at[1, i], peer))
    for copy in sent:
        copy.start()
    def ranked(n):
        high = en - 1 - n
        down = jnp.where(high <= e, high - 1, high)
        return jnp.where(e < en // 2, down, jnp.where(n >= e, n + 1, n))

    def send_own(s):
        for n in range(en - 1):
            along(s, lax.rem(ranked(n) - e + en, en)).start()

    send_own(0)

    for copy in acts:
        copy.wait()

    def prepare(j, carry):
        g = gate[j].astype(f32)
        hid[j] = (g * jax.nn.sigmoid(g) * up[j].astype(f32)).astype(bf16)
        acc[j // 2] = jnp.zeros(acc.shape[1:], f32)
        flat[j // 2] = jnp.zeros(flat.shape[1:], f32)
        return carry

    lax.fori_loop(0, local, prepare, 0)

    def pass_on(s, first, last):
        for n in range(first, last):
            k = lax.rem(e - ranked(en - 2 - n) + en, en)
            along(s, k).wait_recv()
            over(s, k).start()
            mate_own(s, k).start()

    pass_on(0, 0, 1)
    send_own(1)
    pass_on(0, 1, en - 2)
    for copy in sent:
        copy.wait_recv()

    spot = lax.broadcasted_iota(jnp.int32, (total, total), 0)
    lane = lax.broadcasted_iota(jnp.int32, (total, total), 1)
    below = ((spot < lane) & (spot // tokens == lane // tokens)).astype(f32).astype(bf16)
    here = e * local + lax.broadcasted_iota(jnp.int32, (local, total), 0)
    origin = (lax.broadcasted_iota(jnp.int32, (local, total), 1) // tokens * cap).astype(f32)
    top = ids.shape[2]

    def find(which, replica):
        named = jnp.zeros((local, total), f32)
        carried = jnp.zeros((local, total), f32)
        id_all = jnp.concatenate([ids[b, replica] for b in range(en)], axis=1)
        pr_all = jnp.concatenate([probs[b, replica].astype(f32) for b in range(en)], axis=1)
        for k in range(top):
            hit = id_all[k : k + 1, :] == here
            named = jnp.where(hit, 1.0, named)
            carried = jnp.where(hit, pr_all[k : k + 1, :], carried)
        position = jnp.dot(named.astype(bf16), below, preferred_element_type=f32)
        code = jnp.where(named > 0.0, position + origin, -1.0)
        match = code[:, None, :] == lax.broadcasted_iota(jnp.int32, (local, slots, total), 1).astype(f32)
        one[which] = jnp.where(match, 1.0, 0.0).reshape(local * slots, total).astype(bf16)
        return jnp.sum(jnp.where(match, carried[:, None, :], 0.0), axis=2, keepdims=True)

    prob[...] = find(0, d)
    pass_on(0, en - 2, en - 1)
    send_own(2)
    far_send(0).start()
    hs[...] = (prob[...] * hid[...].astype(f32)).astype(bf16)

    def pick(which, src):
        found = jnp.dot(one[which], src, preferred_element_type=f32)
        return found.reshape(local, slots, region).astype(bf16)

    def store_rows(s, p):
        g = index(s, p) - d * steps
        return pltpu.make_async_copy(
            rows.at[s - per, p],
            rows_out.at[:, pl.ds(0, slots), pl.ds(pl.multiple_of(g * region, region), region)],
            lo.at[s - per, p],
        )

    def own_ready(s):
        for k in range(1, en):
            mate_own(s, k).wait_recv()

    def over_ready(s):
        for k in range(1, en):
            mate_over(s, k).wait_recv()

    def relay(s):
        for k in range(1, en):
            over(s, k).wait_recv()
            mate_over(s, k).start()

    def far_relay(i):
        far_send(i).wait_recv()
        far_over(i).start()
        far_mate(i).start()

    def far_last(i):
        far_over(i).wait_recv()
        far_mate_over(i).start()

    def turn_0():
        own_ready(0)

    def turn_1():
        send_own(3)
        pass_on(1, 0, en - 1)
        far_send(1).start()
        relay(0)
        own_ready(1)

    def turn_2():
        pass_on(2, 0, en - 1)
        hid_send().start()
        over_ready(0)

    def turn_3():
        relay(1)
        own_ready(2)

    def turn_4():
        pass_on(3, 0, en - 1)
        over_ready(1)
        far_relay(0)
        far_relay(1)

    def turn_5():
        relay(2)
        own_ready(3)

    def turn_6():
        relay(3)
        over_ready(2)

    def turn_7():
        over_ready(3)

    turns = [turn_0, turn_1, turn_2, turn_3, turn_4, turn_5, turn_6, turn_7]

    def step(r, carry):
        s, own = turn(r)
        plane_now = jnp.where(own, plane, 1 - plane)
        slot = lax.rem(r, RING)
        for n, arrive in enumerate(turns):
            pl.when(r == n)(arrive)
        weights(r).wait()
        into = rows.at[lax.rem(s, per), plane_now]
        into[...] = pick(0, tok[index(s, plane_now)])

        @pl.when(s >= per)
        def _():
            store_rows(s, plane_now).start()

        def two_experts(i, carry):
            acc[i] += lax.dot_general(
                wbuf[slot, 2 * i], into[2 * i], (((1,), (1,)), ((), ())), preferred_element_type=f32
            )
            flat[i] += lax.dot_general(
                into[2 * i + 1], wbuf[slot, 2 * i + 1], (((1,), (1,)), ((), ())), preferred_element_type=f32
            )
            return carry

        lax.fori_loop(0, local // 2, two_experts, 0, unroll=True)

        @pl.when(r + RING < 2 * steps)
        def _():
            weights(r + RING).start()

        return carry

    lax.fori_loop(0, 2 * steps, step, 0)

    far_last(0)
    column = lax.broadcasted_iota(jnp.int32, (slots, cells.shape[2]), 1)

    def finish(i, dots):
        for j, grad in ((2 * i, acc[i].T), (2 * i + 1, flat[i])):
            gh[j] = grad
            dot = jnp.sum(grad * hid[j].astype(f32), axis=1, keepdims=True)
            dots = jnp.where(column == j, dot, dots)
        return dots

    dots = lax.fori_loop(0, local // 2, finish, jnp.zeros(column.shape, f32), unroll=8)
    for b in range(en):
        cells[b, pl.ds(0, cap), :] = dots[b * cap : (b + 1) * cap, :]
        cells[b, pl.ds(cap, cells.shape[1] - cap), :] = jnp.zeros((cells.shape[1] - cap, cells.shape[2]), f32)
    returns = [
        remote(cells.at[peer[1]], back.at[t, e], rs.at[i], rr.at[i], peer) for i, peer in enumerate(group)
    ]
    for copy in returns:
        copy.start()
    keep = pltpu.make_async_copy(cells.at[e], back.at[t, e], la.at[0])
    keep.start()
    outs = [
        pltpu.make_async_copy(hs, hs_out.at[:, pl.ds(0, slots), :], lx.at[steps]),
        pltpu.make_async_copy(grad_gate, gate_out, lm.at[0]),
        pltpu.make_async_copy(grad_up, up_out, lm.at[1]),
    ]
    outs[0].start()

    def activations(j, carry):
        g = gate[j].astype(f32)
        u = up[j].astype(f32)
        s = jax.nn.sigmoid(g)
        weighted = prob[j] * gh[j]
        grad_up[j] = (weighted * (g * s)).astype(bf16)
        grad_gate[j] = (weighted * u * s * (1.0 + g * (1.0 - s))).astype(bf16)
        return carry

    lax.fori_loop(0, local, activations, 0, unroll=4)
    find(1, far)
    for copy in outs[1:]:
        copy.start()
    far_last(1)
    far_outs = []

    def far_pick(q):
        far_rows[q] = pick(1, oth[q])
        return pltpu.make_async_copy(
            far_rows.at[q],
            rows_out.at[:, pl.ds(slots, slots), pl.ds(pl.multiple_of(q * region, region), region)],
            lx.at[len(far_outs)],
        )

    for i in range(per):
        far_mate(i).wait_recv()
        far_outs.append(far_pick(plane * per + i))
        far_outs[-1].start()
    for i in range(per):
        far_mate_over(i).wait_recv()
        far_outs.append(far_pick((1 - plane) * per + i))
        far_outs[-1].start()
    hid_send().wait_recv()
    copy = pltpu.make_async_copy(hs_far, hs_out.at[:, pl.ds(slots, slots), :], la.at[1])
    copy.start()
    outs.append(copy)

    def drain(s, carry):
        for k in range(1, en):
            along(s, k).wait_send()
            over(s, k).wait_send()
            mate_own(s, k).wait_send()
            mate_over(s, k).wait_send()
        return carry

    lax.fori_loop(0, steps, drain, 0)
    for copy in sent:
        copy.wait_send()
    hid_send().wait_send()
    for i in range(per):
        far_send(i).wait_send()
        far_over(i).wait_send()
        far_mate(i).wait_send()
        far_mate_over(i).wait_send()
        for p in range(2):
            store_rows(per + i, p).wait()
    for copy in returns:
        copy.wait()
    for copy in outs + far_outs + [keep]:
        copy.wait()


def weight_kernel(
    cap, chunk, rows_ref, hs_ref, gate_ref, up_ref, back_ref, ids_ref,
    gate_out, up_out, w_out, probs_out,
    rows, hs, back, ids, grad_gate, grad_up, grad_w, grad_probs,
    sm, sr, sh, so, sg,
):
    f32, bf16 = jnp.float32, jnp.bfloat16
    local = rows.shape[0]
    count = local // chunk

    def part(ref, c):
        return ref.at[pl.ds(c * chunk, chunk)]

    def load(c):
        return pltpu.make_async_copy(part(rows_ref, c), part(rows, c), sr.at[c])

    def load_hs(c):
        return pltpu.make_async_copy(part(hs_ref, c), part(hs, c), sh.at[c])

    def store(j):
        return pltpu.make_async_copy(grad_w.at[j], w_out.at[j], so.at[j])

    small = [(back_ref, back), (ids_ref, ids), (gate_ref, grad_gate), (up_ref, grad_up)]
    small = [pltpu.make_async_copy(a, b, sm.at[n]) for n, (a, b) in enumerate(small)]
    small[0].start()
    small[1].start()
    load_hs(0).start()
    load(0).start()
    small[0].wait()
    small[1].wait()

    top, tokens = ids.shape
    tn, en = back.shape[0], back.shape[1]
    summed = back[0]
    for i in range(1, tn):
        summed = summed + back[i]
    cell = jnp.concatenate([summed[b].T[:local] for b in range(en)], axis=0)
    every = lax.broadcasted_iota(jnp.int32, (en * local, tokens), 0)
    spot = lax.broadcasted_iota(jnp.int32, (tokens, tokens), 0)
    lane = lax.broadcasted_iota(jnp.int32, (tokens, tokens), 1)
    below = (spot < lane).astype(f32).astype(bf16)
    named = jnp.zeros(every.shape, f32)
    for k in range(top):
        named = jnp.where(ids[k : k + 1, :] == every, 1.0, named)
    before = jnp.dot(named.astype(bf16), below, preferred_element_type=f32)
    value = jnp.zeros(every.shape, f32)
    for p in range(cap):
        value = jnp.where(before == float(p), cell[:, p : p + 1], value)
    for k in range(top):
        found = jnp.where(ids[k : k + 1, :] == every, value, 0.0)
        grad_probs[k : k + 1, :] = jnp.sum(found, axis=0, keepdims=True)
    ends = [
        pltpu.make_async_copy(grad_probs, probs_out, sg.at[0]),
        pltpu.make_async_copy(grad_gate, gate_out.at[0], sg.at[1]),
        pltpu.make_async_copy(grad_up, up_out.at[0], sg.at[2]),
    ]
    ends[0].start()
    load_hs(0).wait()
    load(0).wait()
    for c in range(1, count):
        load_hs(c).start()
        load(c).start()
    small[2].start()
    small[3].start()

    def one_chunk(c, carry):
        @pl.when(c > 0)
        def _():
            load_hs(c).wait()
            load(c).wait()

        @pl.when(c == count - 1)
        def _():
            small[2].wait()
            small[3].wait()
            ends[1].start()
            ends[2].start()

        for k in range(chunk):
            j = c * chunk + k
            turned = hs[j].astype(f32).T.astype(bf16)
            grad_w[j] = jnp.dot(turned, rows[j], preferred_element_type=f32).astype(bf16)
            store(j).start()

        return carry

    lax.fori_loop(0, count, one_chunk, 0)

    def stored(j, carry):
        store(j).wait()
        return carry

    lax.fori_loop(0, local, stored, 0)
    for copy in ends:
        copy.wait()


def on_device(grad_out, route_ids, route_probs, gate_act, up_act, w_down):
    tokens, width = grad_out.shape
    top = route_ids.shape[1]
    tn, en, rn = lax.axis_size("tensor"), lax.axis_size("expert"), lax.axis_size("dp")
    local, units, slots = w_down.shape[0], w_down.shape[1], gate_act.shape[2]
    cap = slots // en
    half = width // rn
    steps = 4
    per = steps // 2
    region = width // (2 * steps)
    total = en * tokens
    f32, bf16 = jnp.float32, jnp.bfloat16
    sem = pltpu.SemaphoreType.DMA
    anyspace = pl.BlockSpec(memory_space=pl.ANY)
    ids_turned = route_ids.T
    both = rn * slots
    hidden_shape = (local, slots, units)
    rows, hs, early_gate, early_up, back = pl.pallas_call(
        functools.partial(gather_kernel, (tn, en, rn), cap),
        out_shape=(
            jax.ShapeDtypeStruct((local, both, half), bf16),
            jax.ShapeDtypeStruct((local, both, units), bf16),
            jax.ShapeDtypeStruct(hidden_shape, bf16),
            jax.ShapeDtypeStruct(hidden_shape, bf16),
            jax.ShapeDtypeStruct((tn, en, 8, 128), f32),
        ),
        in_specs=[anyspace] * 6,
        out_specs=(anyspace,) * 5,
        scratch_shapes=[
            pltpu.VMEM((2 * steps, total, region), bf16),
            pltpu.VMEM((steps, total, region), bf16),
            pltpu.VMEM((en, rn, top, tokens), jnp.int32),
            pltpu.VMEM((en, rn, top, tokens), bf16),
            pltpu.VMEM(hidden_shape, bf16),
            pltpu.VMEM(hidden_shape, bf16),
            pltpu.VMEM((RING, local, units, region), bf16),
            pltpu.VMEM((per, 2, local, slots, region), bf16),
            pltpu.VMEM((steps, local, slots, region), bf16),
            pltpu.VMEM((rn, local * slots, total), bf16),
            pltpu.VMEM((local // 2, units, slots), f32),
            pltpu.VMEM((local // 2, slots, units), f32),
            pltpu.VMEM(hidden_shape, f32),
            pltpu.VMEM(hidden_shape, bf16),
            pltpu.VMEM(hidden_shape, bf16),
            pltpu.VMEM(hidden_shape, bf16),
            pltpu.VMEM(hidden_shape, bf16),
            pltpu.VMEM(hidden_shape, bf16),
            pltpu.VMEM((local, slots, 1), f32),
            pltpu.VMEM((en, 8, 128), f32),
            sem((2 * steps,)), sem((2,)), sem((2,)), sem((RING,)), sem((per, 2)),
            sem((steps, en - 1)), sem((steps, en - 1)),
            sem((2, en * rn - 1)), sem((2, en * rn - 1)),
            sem((steps, en - 1)), sem((steps, en - 1)),
            sem((steps, en - 1)), sem((steps, en - 1)),
            sem((steps, en - 1)), sem((steps, en - 1)),
            sem((per,)), sem((per,)), sem((per,)), sem((per,)), sem((per,)), sem((per,)), sem((per,)), sem((per,)),
            sem((2,)), sem((tn * en - 1,)), sem((tn * en - 1,)),
        ],
        compiler_params=pltpu.CompilerParams(
            collective_id=0, has_side_effects=True, vmem_limit_bytes=67043328
        ),
    )(grad_out, ids_turned, route_probs.T, gate_act, up_act, w_down)

    chunk = 8
    grad_gate, grad_up, grad_w, grad_probs = pl.pallas_call(
        functools.partial(weight_kernel, cap, chunk),
        in_specs=[anyspace] * 6,
        out_specs=(anyspace,) * 4,
        out_shape=(
            jax.ShapeDtypeStruct((1,) + hidden_shape, bf16),
            jax.ShapeDtypeStruct((1,) + hidden_shape, bf16),
            jax.ShapeDtypeStruct((local, units, half), bf16),
            jax.ShapeDtypeStruct((top, tokens), f32),
        ),
        scratch_shapes=[
            pltpu.VMEM((local, both, half), bf16),
            pltpu.VMEM((local, both, units), bf16),
            pltpu.VMEM((tn, en, 8, 128), f32),
            pltpu.VMEM((top, tokens), jnp.int32),
            pltpu.VMEM(hidden_shape, bf16),
            pltpu.VMEM(hidden_shape, bf16),
            pltpu.VMEM((local, units, half), bf16),
            pltpu.VMEM((top, tokens), f32),
            sem((4,)), sem((local // chunk,)), sem((local // chunk,)), sem((local,)), sem((3,)),
        ],
        compiler_params=pltpu.CompilerParams(vmem_limit_bytes=67043328),
    )(rows, hs, early_gate, early_up, back, ids_turned)
    return grad_gate, grad_up, grad_w, grad_probs.T


def solution(mesh):
    sizes = mesh.shape
    small = sizes["tensor"] == 4 and sizes["dp"] == 2 and sizes["expert"] <= 8
    placed = (
        P(("expert", "dp"), None),
        P(("expert", "dp"), None),
        P(("expert", "dp"), None),
        P("dp", "expert", None, "tensor"),
        P("dp", "expert", None, "tensor"),
        P("expert", "tensor", None),
    )
    return jax.shard_map(
        on_device if small else on_device_wide,
        mesh=mesh,
        in_specs=placed,
        out_specs=(
            P("dp", "expert", None, "tensor"),
            P("dp", "expert", None, "tensor"),
            P("expert", "tensor", "dp"),
            P(("expert", "dp"), None),
        ),
        check_vma=False,
    )
```

```python
import functools
import jax
import jax.numpy as jnp
from jax import lax
from jax.experimental import pallas as pl
from jax.experimental.pallas import tpu as pltpu
from jax.sharding import PartitionSpec as P


def on_device_wide(grad_out, route_ids, route_probs, gate_act, up_act, w_down):
    tok_count = grad_out.shape[0]
    top_count = route_ids.shape[1]
    expert_count = lax.axis_size("expert")
    tensor_count = lax.axis_size("tensor")
    local_experts = w_down.shape[0]
    experts = local_experts * expert_count
    slot_count = gate_act.shape[2]
    capacity = slot_count // expert_count
    model_width = grad_out.shape[1]
    quarter = model_width // tensor_count
    route_flat = route_ids.reshape(-1)
    expert_iota = lax.broadcasted_iota(jnp.int32, (1, experts), 1)
    matches = (route_flat[:, None] == expert_iota).astype(jnp.int32)
    earlier = jnp.cumsum(matches, axis=0) - matches
    position = jnp.sum(earlier * matches, axis=1)
    target = route_flat * capacity + position
    cell_iota = lax.broadcasted_iota(jnp.int32, (1, experts * capacity), 1)
    chosen = target[:, None] == cell_iota
    chosen_weight = chosen.astype(jnp.float32)
    token_chosen = jnp.sum(
        chosen_weight.reshape(tok_count, top_count, experts * capacity), axis=1
    ).astype(jnp.bfloat16)
    own_columns = lax.dynamic_slice_in_dim(grad_out, lax.axis_index("tensor") * quarter, quarter, 1)
    send_rows = jnp.einsum(
        "nf,nd->fd", token_chosen, own_columns, preferred_element_type=jnp.float32
    ).astype(jnp.bfloat16)
    send_probs = jnp.sum(
        chosen_weight * route_probs.reshape(-1).astype(jnp.float32)[:, None], axis=0
    ).astype(jnp.bfloat16)
    send_rows = send_rows.reshape(expert_count, local_experts, capacity, quarter)
    send_probs = send_probs.reshape(expert_count, local_experts, capacity)
    arrived_rows, arrived_probs = (
        lax.all_to_all(send_rows, "expert", split_axis=0, concat_axis=0, tiled=True),
        lax.all_to_all(send_probs, "expert", split_axis=0, concat_axis=0, tiled=True),
    )
    gathered = lax.all_gather(arrived_rows, "tensor", axis=3, tiled=True)
    slot_rows = jnp.transpose(gathered, (1, 0, 2, 3)).reshape(
        local_experts, slot_count, model_width
    )
    slot_probs = (
        jnp.transpose(arrived_probs, (1, 0, 2))
        .reshape(local_experts, slot_count)
        .astype(jnp.float32)
    )
    gate_pre = gate_act[0].astype(jnp.float32)
    up_pre = up_act[0].astype(jnp.float32)
    grad_hidden = jnp.einsum("jsd,jfd->jsf", slot_rows, w_down, preferred_element_type=jnp.float32)
    sigmoid_gate = jax.nn.sigmoid(gate_pre)
    silu_gate = gate_pre * sigmoid_gate
    hidden = (silu_gate * up_pre).astype(jnp.bfloat16)
    partial_dot = jnp.sum(grad_hidden * hidden.astype(jnp.float32), axis=2)
    grad_scaled = slot_probs[:, :, None] * grad_hidden
    grad_up = (grad_scaled * silu_gate).astype(jnp.bfloat16)
    grad_gate = (
        grad_scaled * up_pre * sigmoid_gate * (1.0 + gate_pre * (1.0 - sigmoid_gate))
    ).astype(jnp.bfloat16)
    scaled_rows = (slot_probs[:, :, None] * slot_rows.astype(jnp.float32)).astype(jnp.bfloat16)
    replica_count = lax.axis_size("dp")
    column_count = model_width // replica_count
    split_rows = jnp.transpose(
        scaled_rows.reshape(local_experts, slot_count, replica_count, column_count), (2, 0, 1, 3)
    )
    columns = lax.all_to_all(split_rows, "dp", split_axis=0, concat_axis=0, tiled=True)
    initial = jnp.zeros((local_experts, hidden.shape[2], column_count), jnp.float32)
    hidden_block = lax.all_gather(hidden[None], "dp", axis=0, tiled=True)

    def add_member(member, summed):
        hid_one = lax.dynamic_index_in_dim(hidden_block, member, 0, keepdims=False)
        col_one = lax.dynamic_index_in_dim(columns, member, 0, keepdims=False)
        term = jnp.einsum("jsf,jsd->jfd", hid_one, col_one, preferred_element_type=jnp.float32)
        rounded = lax.optimization_barrier(term.astype(jnp.bfloat16))
        return summed + rounded.astype(jnp.float32)

    grad_weight = lax.fori_loop(0, hidden_block.shape[0], add_member, initial).astype(jnp.bfloat16)
    prob_cells = jnp.transpose(
        partial_dot.reshape(local_experts, expert_count, capacity), (1, 0, 2)
    )
    prob_cells = lax.psum(prob_cells, "tensor")
    returned = lax.all_to_all(prob_cells, "expert", split_axis=0, concat_axis=0, tiled=True)
    returned_flat = returned.reshape(-1)
    grad_probs = jnp.sum(jnp.where(chosen, returned_flat[None, :], 0.0), axis=1).reshape(
        tok_count, top_count
    )
    return (grad_gate[None], grad_up[None], grad_weight, grad_probs)


MESH = pl.DeviceIdType.MESH
RING = 6


def gather_kernel(
    sizes, cap, x_ref, ids_ref, probs_ref, gate_ref, up_ref, w_ref,
    rows_out, hs_out, gate_out, up_out, back,
    tok, oth, ids, probs, gate, up, wbuf, rows, far_rows, one, acc, flat, gh, hid, hs, hs_far, grad_gate, grad_up, prob, cells,
    lx, lm, la, lw, lo, zs, zr, ms, mr, ys, yr, as_, ar, bs, br, xs, xr, qs, qr, hsem, rs, rr,
):
    tn, en, rn = sizes
    f32, bf16 = jnp.float32, jnp.bfloat16
    t, e, d = lax.axis_index("tensor"), lax.axis_index("expert"), lax.axis_index("dp")
    plane, core = t // 2, lax.rem(t, 2)
    across = lax.rem(t + 2, tn)
    mate = t + 1 - 2 * core
    far = 1 - d
    steps = tok.shape[0] // 2
    per = steps // 2
    tokens, width = x_ref.shape
    region = tok.shape[2]
    piece = region // 2
    local, slots, units = gh.shape
    total = en * tokens

    def block(k):
        return lax.rem(e - k + en, en)

    def index(s, p):
        half = jnp.where(s < per, far, d)
        return half * steps + p * per + lax.rem(s, per)

    def part(buf, g, b, q):
        return buf.at[g, pl.ds(pl.multiple_of(b * tokens, tokens), tokens), pl.ds(pl.multiple_of(q * piece, piece), piece)]

    def wide_part(buf, g, q):
        return buf.at[g, :, pl.ds(pl.multiple_of(q * piece, piece), piece)]

    def remote(src, dst, ssem, rsem, peer):
        return pltpu.make_async_remote_copy(
            src_ref=src, dst_ref=dst, send_sem=ssem, recv_sem=rsem, device_id=peer, device_id_type=MESH
        )

    def along(s, k):
        ref = part(tok, index(s, plane), e, core)
        return remote(ref, ref, zs.at[s, k - 1], zr.at[s, k - 1], (t, lax.rem(e + k, en), d))

    def over(s, k):
        ref = part(tok, index(s, plane), block(k), core)
        return remote(ref, ref, ys.at[s, k - 1], yr.at[s, k - 1], (across, e, d))

    def mate_own(s, k):
        ref = part(tok, index(s, plane), block(k), core)
        return remote(ref, ref, as_.at[s, k - 1], ar.at[s, k - 1], (mate, e, d))

    def mate_over(s, k):
        ref = part(tok, index(s, 1 - plane), block(k), core)
        return remote(ref, ref, bs.at[s, k - 1], br.at[s, k - 1], (mate, e, d))

    def far_send(q, i):
        p = plane if q == 0 else 1 - plane
        return remote(
            wide_part(tok, index(i, p), core), wide_part(oth, p * per + i, core), xs.at[q, i], xr.at[q, i], (t, e, far)
        )

    def far_over():
        ref = wide_part(oth, plane * per + per - 1, core)
        return remote(ref, ref, xs.at[1, per - 1], xr.at[1, per - 1], (across, e, d))

    def far_mate(q, i):
        ref = wide_part(oth, (plane if q == 0 else 1 - plane) * per + i, core)
        return remote(ref, ref, qs.at[q, i], qr.at[q, i], (mate, e, d))

    def hid_send():
        return remote(hs, hs_far, hsem.at[0], hsem.at[1], (t, e, far))

    def turn(r):
        own = (r == 0) | ((lax.rem(r, 2) == 1) & (r < 2 * steps - 1))
        s = jnp.where(r == 0, 0, jnp.where(own, (r + 1) // 2, jnp.where(r == 2 * steps - 1, steps - 1, r // 2 - 1)))
        return s, own

    def weights(r):
        s, own = turn(r)
        g = index(s, jnp.where(own, plane, 1 - plane))
        slot = lax.rem(r, RING)
        return pltpu.make_async_copy(
            w_ref.at[:, :, pl.ds(pl.multiple_of(g * region, region), region)], wbuf.at[slot], lw.at[slot]
        )

    def load_own(g):
        return pltpu.make_async_copy(
            x_ref.at[:, pl.ds(g * region, region)],
            tok.at[g, pl.ds(pl.multiple_of(e * tokens, tokens), tokens), :], lx.at[g],
        )

    loads = [load_own(g) for g in range(2 * steps)]
    metas = [
        pltpu.make_async_copy(ids_ref, ids.at[e, d], lm.at[0]),
        pltpu.make_async_copy(probs_ref, probs.at[e, d], lm.at[1]),
    ]
    acts = [pltpu.make_async_copy(gate_ref.at[0], gate, la.at[0]), pltpu.make_async_copy(up_ref.at[0], up, la.at[1])]
    for copy in metas + loads + acts:
        copy.start()

    others = []
    for i in range(en):
        for j in range(rn):
            if i or j:
                others.append((t, lax.rem(e + i, en), lax.rem(d + j, rn)))
    group = []
    for i in range(tn):
        for j in range(en):
            if i or j:
                group.append((lax.rem(t + i, tn), lax.rem(e + j, en), d))
    greet = group + [peer for n, peer in enumerate(others) if (n + 1) % rn]
    barrier = pltpu.get_barrier_semaphore()
    for peer in greet:
        pl.semaphore_signal(barrier, inc=1, device_id=peer, device_id_type=MESH)
    for copy in metas + loads:
        copy.wait()
    for r in range(RING):
        weights(r).start()
    pl.semaphore_wait(barrier, len(greet))

    sent = []
    for i, peer in enumerate(others):
        sent.append(remote(ids.at[e, d], ids.at[e, d], ms.at[0, i], mr.at[0, i], peer))
        sent.append(remote(probs.at[e, d], probs.at[e, d], ms.at[1, i], mr.at[1, i], peer))
    def ranked(n):
        high = en - 1 - n
        down = jnp.where(high <= e, high - 1, high)
        return jnp.where(e < en // 2, down, jnp.where(n >= e, n + 1, n))

    def send_own(s):
        for n in range(en - 1):
            along(s, lax.rem(ranked(n) - e + en, en)).start()

    send_own(0)
    for copy in sent:
        copy.start()

    for copy in acts:
        copy.wait()

    def prepare(j, carry):
        g = gate[j].astype(f32)
        hid[j] = (g * jax.nn.sigmoid(g) * up[j].astype(f32)).astype(bf16)
        for q in range(2):
            acc[q, j // 2] = jnp.zeros(acc.shape[2:], f32)
            flat[q, j // 2] = jnp.zeros(flat.shape[2:], f32)
        return carry

    lax.fori_loop(0, local, prepare, 0)

    def pass_on(s, first, last):
        for n in range(first, last):
            k = lax.rem(e - ranked(en - 2 - n) + en, en)
            along(s, k).wait_recv()
            over(s, k).start()
            mate_own(s, k).start()

    pass_on(0, 0, 1)
    send_own(1)
    pass_on(0, 1, en - 2)
    for copy in sent:
        copy.wait_recv()

    spot = lax.broadcasted_iota(jnp.int32, (total, total), 0)
    lane = lax.broadcasted_iota(jnp.int32, (total, total), 1)
    below = ((spot < lane) & (spot // tokens == lane // tokens)).astype(f32).astype(bf16)
    here = e * local + lax.broadcasted_iota(jnp.int32, (local, total), 0)
    origin = (lax.broadcasted_iota(jnp.int32, (local, total), 1) // tokens * cap).astype(f32)
    top = ids.shape[2]

    def find(which, replica):
        named = jnp.zeros((local, total), f32)
        carried = jnp.zeros((local, total), f32)
        id_all = jnp.concatenate([ids[b, replica] for b in range(en)], axis=1)
        pr_all = jnp.concatenate([probs[b, replica].astype(f32) for b in range(en)], axis=1)
        for k in range(top):
            hit = id_all[k : k + 1, :] == here
            named = jnp.where(hit, 1.0, named)
            carried = jnp.where(hit, pr_all[k : k + 1, :], carried)
        position = jnp.dot(named.astype(bf16), below, preferred_element_type=f32)
        code = jnp.where(named > 0.0, position + origin, -1.0)
        match = code[:, None, :] == lax.broadcasted_iota(jnp.int32, (local, slots, total), 1).astype(f32)
        one[which] = jnp.where(match, 1.0, 0.0).reshape(local * slots, total).astype(bf16)
        return jnp.sum(jnp.where(match, carried[:, None, :], 0.0), axis=2, keepdims=True)

    prob[...] = find(0, d)
    pass_on(0, en - 2, en - 1)
    send_own(2)
    far_send(0, 0).start()
    hs[...] = (prob[...] * hid[...].astype(f32)).astype(bf16)

    def pick(which, src):
        found = jnp.dot(one[which], src, preferred_element_type=f32)
        return found.reshape(local, slots, region).astype(bf16)

    def store_rows(s, p):
        g = index(s, p) - d * steps
        return pltpu.make_async_copy(
            rows.at[s - per, p],
            rows_out.at[:, pl.ds(0, slots), pl.ds(pl.multiple_of(g * region, region), region)],
            lo.at[s - per, p],
        )

    def own_ready(s):
        for k in range(1, en):
            mate_own(s, k).wait_recv()

    def over_ready(s):
        for k in range(1, en):
            mate_over(s, k).wait_recv()

    def relay(s):
        for k in range(1, en):
            over(s, k).wait_recv()
            mate_over(s, k).start()

    def far_relay(q, i):
        far_send(q, i).wait_recv()
        far_mate(q, i).start()

    def turn_0():
        own_ready(0)

    def turn_1():
        send_own(3)
        pass_on(1, 0, en - 1)
        far_send(0, 1).start()
        relay(0)
        far_send(1, 0).start()
        own_ready(1)

    def turn_2():
        pass_on(2, 0, en - 1)
        hid_send().start()
        over_ready(0)

    def turn_3():
        relay(1)
        own_ready(2)

    def turn_4():
        pass_on(3, 0, en - 1)
        over_ready(1)
        far_relay(0, 0)

    def turn_5():
        relay(2)
        own_ready(3)
        far_relay(0, 1)
        far_over().start()

    def turn_6():
        relay(3)
        over_ready(2)

    def turn_7():
        over_ready(3)
        far_relay(1, 0)

    turns = [turn_0, turn_1, turn_2, turn_3, turn_4, turn_5, turn_6, turn_7]

    def step(r, carry):
        s, own = turn(r)
        plane_now = jnp.where(own, plane, 1 - plane)
        slot = lax.rem(r, RING)
        for n, arrive in enumerate(turns):
            pl.when(r == n)(arrive)
        weights(r).wait()
        into = rows.at[lax.rem(s, per), plane_now]
        into[...] = pick(0, tok[index(s, plane_now)])

        @pl.when(s >= per)
        def _():
            store_rows(s, plane_now).start()

        def product(a, b):
            return lax.dot_general(a, b, (((1,), (1,)), ((), ())), preferred_element_type=f32)

        def two_experts(i, carry):
            for q in range(2):
                cols = slice(q * piece, (q + 1) * piece)
                acc[q, i] += product(wbuf[slot, 2 * i, :, cols], into[2 * i, :, cols])
            for q in range(2):
                cols = slice(q * piece, (q + 1) * piece)
                flat[q, i] += product(into[2 * i + 1, :, cols], wbuf[slot, 2 * i + 1, :, cols])
            return carry

        lax.fori_loop(0, local // 2, two_experts, 0, unroll=True)

        @pl.when(r + RING < 2 * steps)
        def _():
            weights(r + RING).start()

        return carry

    lax.fori_loop(0, 2 * steps, step, 0)

    far_over().wait_recv()
    far_mate(1, per - 1).start()
    column = lax.broadcasted_iota(jnp.int32, (slots, cells.shape[2]), 1)

    def finish(i, dots):
        for j, grad in ((2 * i, (acc[0, i] + acc[1, i]).T), (2 * i + 1, flat[0, i] + flat[1, i])):
            gh[j] = grad
            dot = jnp.sum(grad * hid[j].astype(f32), axis=1, keepdims=True)
            dots = jnp.where(column == j, dot, dots)
        return dots

    dots = lax.fori_loop(0, local // 2, finish, jnp.zeros(column.shape, f32), unroll=8)
    for b in range(en):
        cells[b, pl.ds(0, cap), :] = dots[b * cap : (b + 1) * cap, :]
        cells[b, pl.ds(cap, cells.shape[1] - cap), :] = jnp.zeros((cells.shape[1] - cap, cells.shape[2]), f32)
    returns = [
        remote(cells.at[peer[1]], back.at[t, e], rs.at[i], rr.at[i], peer) for i, peer in enumerate(group)
    ]
    for copy in returns:
        copy.start()
    keep = pltpu.make_async_copy(cells.at[e], back.at[t, e], la.at[0])
    keep.start()
    outs = [
        pltpu.make_async_copy(hs, hs_out.at[:, pl.ds(0, slots), :], lx.at[steps]),
        pltpu.make_async_copy(grad_gate, gate_out, lm.at[0]),
        pltpu.make_async_copy(grad_up, up_out, lm.at[1]),
    ]
    outs[0].start()

    def activations(j, carry):
        g = gate[j].astype(f32)
        u = up[j].astype(f32)
        s = jax.nn.sigmoid(g)
        weighted = prob[j] * gh[j]
        grad_up[j] = (weighted * (g * s)).astype(bf16)
        grad_gate[j] = (weighted * u * s * (1.0 + g * (1.0 - s))).astype(bf16)
        return carry

    lax.fori_loop(0, local, activations, 0, unroll=4)
    find(1, far)
    for copy in outs[1:]:
        copy.start()
    far_outs = []
    for i in range(steps):
        far_mate(i // per, i % per).wait_recv()
        q = (plane if i < per else 1 - plane) * per + i % per
        far_rows[q] = pick(1, oth[q])
        far_outs.append(
            pltpu.make_async_copy(
                far_rows.at[q],
                rows_out.at[:, pl.ds(slots, slots), pl.ds(pl.multiple_of(q * region, region), region)],
                lx.at[i],
            )
        )
        far_outs[-1].start()
    hid_send().wait_recv()
    copy = pltpu.make_async_copy(hs_far, hs_out.at[:, pl.ds(slots, slots), :], la.at[1])
    copy.start()
    outs.append(copy)

    def drain(s, carry):
        for k in range(1, en):
            along(s, k).wait_send()
            over(s, k).wait_send()
            mate_own(s, k).wait_send()
            mate_over(s, k).wait_send()
        return carry

    lax.fori_loop(0, steps, drain, 0)
    for copy in sent:
        copy.wait_send()
    hid_send().wait_send()
    for i in range(per):
        for p in range(2):
            far_send(p, i).wait_send()
            far_mate(p, i).wait_send()
            store_rows(per + i, p).wait()
    for copy in returns:
        copy.wait()
    for copy in outs + far_outs + [keep]:
        copy.wait()


def weight_kernel(
    cap, chunk, rows_ref, hs_ref, gate_ref, up_ref, back_ref, ids_ref,
    gate_out, up_out, w_out, probs_out,
    rows, hs, back, ids, grad_gate, grad_up, grad_w, grad_probs,
    sm, sr, sh, so, sg,
):
    f32, bf16 = jnp.float32, jnp.bfloat16
    local = rows.shape[0]
    count = local // chunk

    def part(ref, c):
        return ref.at[pl.ds(c * chunk, chunk)]

    def load(c):
        return pltpu.make_async_copy(part(rows_ref, c), part(rows, c), sr.at[c])

    def load_hs(c):
        return pltpu.make_async_copy(part(hs_ref, c), part(hs, c), sh.at[c])

    def store(j):
        return pltpu.make_async_copy(grad_w.at[j], w_out.at[j], so.at[j])

    small = [(back_ref, back), (ids_ref, ids), (gate_ref, grad_gate), (up_ref, grad_up)]
    small = [pltpu.make_async_copy(a, b, sm.at[n]) for n, (a, b) in enumerate(small)]
    load_hs(0).start()
    load(0).start()
    ends = [
        pltpu.make_async_copy(grad_probs, probs_out, sg.at[0]),
        pltpu.make_async_copy(grad_gate, gate_out.at[0], sg.at[1]),
        pltpu.make_async_copy(grad_up, up_out.at[0], sg.at[2]),
    ]
    load_hs(0).wait()
    load(0).wait()
    for c in range(1, count):
        load_hs(c).start()
        load(c).start()
    for copy in small:
        copy.start()

    def one_chunk(c, carry):
        @pl.when(c > 0)
        def _():
            load_hs(c).wait()
            load(c).wait()

        @pl.when(c == count - 1)
        def _():
            small[2].wait()
            small[3].wait()
            ends[1].start()
            ends[2].start()

        for k in range(chunk):
            j = c * chunk + k
            turned = hs[j].astype(f32).T.astype(bf16)
            grad_w[j] = jnp.dot(turned, rows[j], preferred_element_type=f32).astype(bf16)
            store(j).start()

        return carry

    lax.fori_loop(0, count, one_chunk, 0)

    small[0].wait()
    small[1].wait()
    top, tokens = ids.shape
    tn, en = back.shape[0], back.shape[1]
    summed = back[0]
    for i in range(1, tn):
        summed = summed + back[i]
    cell = jnp.concatenate([summed[b].T[:local] for b in range(en)], axis=0)
    every = lax.broadcasted_iota(jnp.int32, (en * local, tokens), 0)
    spot = lax.broadcasted_iota(jnp.int32, (tokens, tokens), 0)
    lane = lax.broadcasted_iota(jnp.int32, (tokens, tokens), 1)
    below = (spot < lane).astype(f32).astype(bf16)
    named = jnp.zeros(every.shape, f32)
    for k in range(top):
        named = jnp.where(ids[k : k + 1, :] == every, 1.0, named)
    before = jnp.dot(named.astype(bf16), below, preferred_element_type=f32)
    value = jnp.zeros(every.shape, f32)
    for p in range(cap):
        value = jnp.where(before == float(p), cell[:, p : p + 1], value)
    for k in range(top):
        found = jnp.where(ids[k : k + 1, :] == every, value, 0.0)
        grad_probs[k : k + 1, :] = jnp.sum(found, axis=0, keepdims=True)
    ends[0].start()

    def stored(j, carry):
        store(j).wait()
        return carry

    lax.fori_loop(0, local, stored, 0)
    for copy in ends:
        copy.wait()


def on_device(grad_out, route_ids, route_probs, gate_act, up_act, w_down):
    tokens, width = grad_out.shape
    top = route_ids.shape[1]
    tn, en, rn = lax.axis_size("tensor"), lax.axis_size("expert"), lax.axis_size("dp")
    local, units, slots = w_down.shape[0], w_down.shape[1], gate_act.shape[2]
    cap = slots // en
    half = width // rn
    steps = 4
    per = steps // 2
    region = width // (2 * steps)
    total = en * tokens
    f32, bf16 = jnp.float32, jnp.bfloat16
    sem = pltpu.SemaphoreType.DMA
    anyspace = pl.BlockSpec(memory_space=pl.ANY)
    ids_turned = route_ids.T
    both = rn * slots
    hidden_shape = (local, slots, units)
    rows, hs, early_gate, early_up, back = pl.pallas_call(
        functools.partial(gather_kernel, (tn, en, rn), cap),
        out_shape=(
            jax.ShapeDtypeStruct((local, both, half), bf16),
            jax.ShapeDtypeStruct((local, both, units), bf16),
            jax.ShapeDtypeStruct(hidden_shape, bf16),
            jax.ShapeDtypeStruct(hidden_shape, bf16),
            jax.ShapeDtypeStruct((tn, en, 8, 128), f32),
        ),
        in_specs=[anyspace] * 6,
        out_specs=(anyspace,) * 5,
        scratch_shapes=[
            pltpu.VMEM((2 * steps, total, region), bf16),
            pltpu.VMEM((steps, total, region), bf16),
            pltpu.VMEM((en, rn, top, tokens), jnp.int32),
            pltpu.VMEM((en, rn, top, tokens), bf16),
            pltpu.VMEM(hidden_shape, bf16),
            pltpu.VMEM(hidden_shape, bf16),
            pltpu.VMEM((RING, local, units, region), bf16),
            pltpu.VMEM((per, 2, local, slots, region), bf16),
            pltpu.VMEM((steps, local, slots, region), bf16),
            pltpu.VMEM((rn, local * slots, total), bf16),
            pltpu.VMEM((2, local // 2, units, slots), f32),
            pltpu.VMEM((2, local // 2, slots, units), f32),
            pltpu.VMEM(hidden_shape, f32),
            pltpu.VMEM(hidden_shape, bf16),
            pltpu.VMEM(hidden_shape, bf16),
            pltpu.VMEM(hidden_shape, bf16),
            pltpu.VMEM(hidden_shape, bf16),
            pltpu.VMEM(hidden_shape, bf16),
            pltpu.VMEM((local, slots, 1), f32),
            pltpu.VMEM((en, 8, 128), f32),
            sem((2 * steps,)), sem((2,)), sem((2,)), sem((RING,)), sem((per, 2)),
            sem((steps, en - 1)), sem((steps, en - 1)),
            sem((2, en * rn - 1)), sem((2, en * rn - 1)),
            sem((steps, en - 1)), sem((steps, en - 1)),
            sem((steps, en - 1)), sem((steps, en - 1)),
            sem((steps, en - 1)), sem((steps, en - 1)),
            sem((2, per)), sem((2, per)), sem((2, per)), sem((2, per)),
            sem((2,)), sem((tn * en - 1,)), sem((tn * en - 1,)),
        ],
        compiler_params=pltpu.CompilerParams(
            collective_id=0, has_side_effects=True, vmem_limit_bytes=67043328
        ),
    )(grad_out, ids_turned, route_probs.T, gate_act, up_act, w_down)

    chunk = 8
    grad_gate, grad_up, grad_w, grad_probs = pl.pallas_call(
        functools.partial(weight_kernel, cap, chunk),
        in_specs=[anyspace] * 6,
        out_specs=(anyspace,) * 4,
        out_shape=(
            jax.ShapeDtypeStruct((1,) + hidden_shape, bf16),
            jax.ShapeDtypeStruct((1,) + hidden_shape, bf16),
            jax.ShapeDtypeStruct((local, units, half), bf16),
            jax.ShapeDtypeStruct((top, tokens), f32),
        ),
        scratch_shapes=[
            pltpu.VMEM((local, both, half), bf16),
            pltpu.VMEM((local, both, units), bf16),
            pltpu.VMEM((tn, en, 8, 128), f32),
            pltpu.VMEM((top, tokens), jnp.int32),
            pltpu.VMEM(hidden_shape, bf16),
            pltpu.VMEM(hidden_shape, bf16),
            pltpu.VMEM((local, units, half), bf16),
            pltpu.VMEM((top, tokens), f32),
            sem((4,)), sem((local // chunk,)), sem((local // chunk,)), sem((local,)), sem((3,)),
        ],
        compiler_params=pltpu.CompilerParams(vmem_limit_bytes=67043328),
    )(rows, hs, early_gate, early_up, back, ids_turned)
    return grad_gate, grad_up, grad_w, grad_probs.T


def solution(mesh):
    sizes = mesh.shape
    small = sizes["tensor"] == 4 and sizes["dp"] == 2 and sizes["expert"] <= 8
    placed = (
        P(("expert", "dp"), None),
        P(("expert", "dp"), None),
        P(("expert", "dp"), None),
        P("dp", "expert", None, "tensor"),
        P("dp", "expert", None, "tensor"),
        P("expert", "tensor", None),
    )
    return jax.shard_map(
        on_device if small else on_device_wide,
        mesh=mesh,
        in_specs=placed,
        out_specs=(
            P("dp", "expert", None, "tensor"),
            P("dp", "expert", None, "tensor"),
            P("expert", "tensor", "dp"),
            P(("expert", "dp"), None),
        ),
        check_vma=False,
    )
```

```python
import functools
import jax
import jax.numpy as jnp
from jax import lax
from jax.experimental import pallas as pl
from jax.experimental.pallas import tpu as pltpu
from jax.sharding import PartitionSpec as P


def on_device_wide(grad_out, route_ids, route_probs, gate_act, up_act, w_down):
    tok_count = grad_out.shape[0]
    top_count = route_ids.shape[1]
    expert_count = lax.axis_size("expert")
    tensor_count = lax.axis_size("tensor")
    local_experts = w_down.shape[0]
    experts = local_experts * expert_count
    slot_count = gate_act.shape[2]
    capacity = slot_count // expert_count
    model_width = grad_out.shape[1]
    quarter = model_width // tensor_count
    route_flat = route_ids.reshape(-1)
    expert_iota = lax.broadcasted_iota(jnp.int32, (1, experts), 1)
    matches = (route_flat[:, None] == expert_iota).astype(jnp.int32)
    earlier = jnp.cumsum(matches, axis=0) - matches
    position = jnp.sum(earlier * matches, axis=1)
    target = route_flat * capacity + position
    cell_iota = lax.broadcasted_iota(jnp.int32, (1, experts * capacity), 1)
    chosen = target[:, None] == cell_iota
    chosen_weight = chosen.astype(jnp.float32)
    token_chosen = jnp.sum(
        chosen_weight.reshape(tok_count, top_count, experts * capacity), axis=1
    ).astype(jnp.bfloat16)
    own_columns = lax.dynamic_slice_in_dim(grad_out, lax.axis_index("tensor") * quarter, quarter, 1)
    send_rows = jnp.einsum(
        "nf,nd->fd", token_chosen, own_columns, preferred_element_type=jnp.float32
    ).astype(jnp.bfloat16)
    send_probs = jnp.sum(
        chosen_weight * route_probs.reshape(-1).astype(jnp.float32)[:, None], axis=0
    ).astype(jnp.bfloat16)
    send_rows = send_rows.reshape(expert_count, local_experts, capacity, quarter)
    send_probs = send_probs.reshape(expert_count, local_experts, capacity)
    arrived_rows, arrived_probs = (
        lax.all_to_all(send_rows, "expert", split_axis=0, concat_axis=0, tiled=True),
        lax.all_to_all(send_probs, "expert", split_axis=0, concat_axis=0, tiled=True),
    )
    gathered = lax.all_gather(arrived_rows, "tensor", axis=3, tiled=True)
    slot_rows = jnp.transpose(gathered, (1, 0, 2, 3)).reshape(
        local_experts, slot_count, model_width
    )
    slot_probs = (
        jnp.transpose(arrived_probs, (1, 0, 2))
        .reshape(local_experts, slot_count)
        .astype(jnp.float32)
    )
    gate_pre = gate_act[0].astype(jnp.float32)
    up_pre = up_act[0].astype(jnp.float32)
    grad_hidden = jnp.einsum("jsd,jfd->jsf", slot_rows, w_down, preferred_element_type=jnp.float32)
    sigmoid_gate = jax.nn.sigmoid(gate_pre)
    silu_gate = gate_pre * sigmoid_gate
    hidden = (silu_gate * up_pre).astype(jnp.bfloat16)
    partial_dot = jnp.sum(grad_hidden * hidden.astype(jnp.float32), axis=2)
    grad_scaled = slot_probs[:, :, None] * grad_hidden
    grad_up = (grad_scaled * silu_gate).astype(jnp.bfloat16)
    grad_gate = (
        grad_scaled * up_pre * sigmoid_gate * (1.0 + gate_pre * (1.0 - sigmoid_gate))
    ).astype(jnp.bfloat16)
    scaled_rows = (slot_probs[:, :, None] * slot_rows.astype(jnp.float32)).astype(jnp.bfloat16)
    replica_count = lax.axis_size("dp")
    column_count = model_width // replica_count
    split_rows = jnp.transpose(
        scaled_rows.reshape(local_experts, slot_count, replica_count, column_count), (2, 0, 1, 3)
    )
    columns = lax.all_to_all(split_rows, "dp", split_axis=0, concat_axis=0, tiled=True)
    initial = jnp.zeros((local_experts, hidden.shape[2], column_count), jnp.float32)
    hidden_block = lax.all_gather(hidden[None], "dp", axis=0, tiled=True)

    def add_member(member, summed):
        hid_one = lax.dynamic_index_in_dim(hidden_block, member, 0, keepdims=False)
        col_one = lax.dynamic_index_in_dim(columns, member, 0, keepdims=False)
        term = jnp.einsum("jsf,jsd->jfd", hid_one, col_one, preferred_element_type=jnp.float32)
        rounded = lax.optimization_barrier(term.astype(jnp.bfloat16))
        return summed + rounded.astype(jnp.float32)

    grad_weight = lax.fori_loop(0, hidden_block.shape[0], add_member, initial).astype(jnp.bfloat16)
    prob_cells = jnp.transpose(
        partial_dot.reshape(local_experts, expert_count, capacity), (1, 0, 2)
    )
    prob_cells = lax.psum(prob_cells, "tensor")
    returned = lax.all_to_all(prob_cells, "expert", split_axis=0, concat_axis=0, tiled=True)
    returned_flat = returned.reshape(-1)
    grad_probs = jnp.sum(jnp.where(chosen, returned_flat[None, :], 0.0), axis=1).reshape(
        tok_count, top_count
    )
    return (grad_gate[None], grad_up[None], grad_weight, grad_probs)


MESH = pl.DeviceIdType.MESH
RING = 6


def gather_kernel(
    sizes, cap, x_ref, ids_ref, probs_ref, gate_ref, up_ref, w_ref,
    rows_out, hs_out, gate_out, up_out, back,
    tok, oth, ids, probs, gate, up, wbuf, rows, far_rows, one, acc, flat, gh, hid, hs, hs_far, grad_gate, grad_up, prob, cells,
    lx, lm, la, lw, lo, zs, zr, ms, mr, ys, yr, as_, ar, bs, br, xs, xr, qs, qr, hsem, rs, rr,
):
    tn, en, rn = sizes
    f32, bf16 = jnp.float32, jnp.bfloat16
    t, e, d = lax.axis_index("tensor"), lax.axis_index("expert"), lax.axis_index("dp")
    plane, core = t // 2, lax.rem(t, 2)
    across = lax.rem(t + 2, tn)
    mate = t + 1 - 2 * core
    far = 1 - d
    steps = tok.shape[0] // 2
    per = steps // 2
    tokens, width = x_ref.shape
    region = tok.shape[2]
    piece = region // 2
    local, slots, units = gh.shape
    total = en * tokens

    def block(k):
        return lax.rem(e - k + en, en)

    def index(s, p):
        half = jnp.where(s < per, far, d)
        return half * steps + p * per + lax.rem(s, per)

    def part(buf, g, b, q):
        return buf.at[g, pl.ds(pl.multiple_of(b * tokens, tokens), tokens), pl.ds(pl.multiple_of(q * piece, piece), piece)]

    def wide_part(buf, g, q):
        return buf.at[g, :, pl.ds(pl.multiple_of(q * piece, piece), piece)]

    def remote(src, dst, ssem, rsem, peer):
        return pltpu.make_async_remote_copy(
            src_ref=src, dst_ref=dst, send_sem=ssem, recv_sem=rsem, device_id=peer, device_id_type=MESH
        )

    def along(s, k):
        ref = part(tok, index(s, plane), e, core)
        return remote(ref, ref, zs.at[s, k - 1], zr.at[s, k - 1], (t, lax.rem(e + k, en), d))

    def over(s, k):
        ref = part(tok, index(s, plane), block(k), core)
        return remote(ref, ref, ys.at[s, k - 1], yr.at[s, k - 1], (across, e, d))

    def mate_own(s, k):
        ref = part(tok, index(s, plane), block(k), core)
        return remote(ref, ref, as_.at[s, k - 1], ar.at[s, k - 1], (mate, e, d))

    def mate_over(s, k):
        ref = part(tok, index(s, 1 - plane), block(k), core)
        return remote(ref, ref, bs.at[s, k - 1], br.at[s, k - 1], (mate, e, d))

    def far_send(q, i):
        p = plane if q == 0 else 1 - plane
        return remote(
            wide_part(tok, index(i, p), core), wide_part(oth, p * per + i, core), xs.at[q, i], xr.at[q, i], (t, e, far)
        )

    def far_over():
        ref = wide_part(oth, plane * per + per - 1, core)
        return remote(ref, ref, xs.at[1, per - 1], xr.at[1, per - 1], (across, e, d))

    def far_mate(q, i):
        ref = wide_part(oth, (plane if q == 0 else 1 - plane) * per + i, core)
        return remote(ref, ref, qs.at[q, i], qr.at[q, i], (mate, e, d))

    def hid_send():
        return remote(hs, hs_far, hsem.at[0], hsem.at[1], (t, e, far))

    def turn(r):
        own = (r == 0) | ((lax.rem(r, 2) == 1) & (r < 2 * steps - 1))
        s = jnp.where(r == 0, 0, jnp.where(own, (r + 1) // 2, jnp.where(r == 2 * steps - 1, steps - 1, r // 2 - 1)))
        return s, own

    def weights(r):
        s, own = turn(r)
        g = index(s, jnp.where(own, plane, 1 - plane))
        slot = lax.rem(r, RING)
        return pltpu.make_async_copy(
            w_ref.at[:, :, pl.ds(pl.multiple_of(g * region, region), region)], wbuf.at[slot], lw.at[slot]
        )

    def load_own(g):
        return pltpu.make_async_copy(
            x_ref.at[:, pl.ds(g * region, region)],
            tok.at[g, pl.ds(pl.multiple_of(e * tokens, tokens), tokens), :], lx.at[g],
        )

    loads = [load_own(g) for g in range(2 * steps)]
    metas = [
        pltpu.make_async_copy(ids_ref, ids.at[e, d], lm.at[0]),
        pltpu.make_async_copy(probs_ref, probs.at[e, d], lm.at[1]),
    ]
    acts = [pltpu.make_async_copy(gate_ref.at[0], gate, la.at[0]), pltpu.make_async_copy(up_ref.at[0], up, la.at[1])]
    for copy in metas + loads + acts:
        copy.start()

    others = []
    for i in range(en):
        for j in range(rn):
            if i or j:
                others.append((t, lax.rem(e + i, en), lax.rem(d + j, rn)))
    group = []
    for i in range(tn):
        for j in range(en):
            if i or j:
                group.append((lax.rem(t + i, tn), lax.rem(e + j, en), d))
    greet = group + [peer for n, peer in enumerate(others) if (n + 1) % rn]
    barrier = pltpu.get_barrier_semaphore()
    for peer in greet:
        pl.semaphore_signal(barrier, inc=1, device_id=peer, device_id_type=MESH)
    for copy in metas + loads:
        copy.wait()
    for r in range(RING):
        weights(r).start()
    pl.semaphore_wait(barrier, len(greet))

    sent = []
    for i, peer in enumerate(others):
        sent.append(remote(ids.at[e, d], ids.at[e, d], ms.at[0, i], mr.at[0, i], peer))
        sent.append(remote(probs.at[e, d], probs.at[e, d], ms.at[1, i], mr.at[1, i], peer))
    def ranked(n):
        high = en - 1 - n
        down = jnp.where(high <= e, high - 1, high)
        return jnp.where(e < en // 2, down, jnp.where(n >= e, n + 1, n))

    def send_own(s):
        for n in range(en - 1):
            along(s, lax.rem(ranked(n) - e + en, en)).start()

    send_own(0)
    for copy in sent:
        copy.start()

    for copy in acts:
        copy.wait()

    def prepare(j, carry):
        g = gate[j].astype(f32)
        hid[j] = (g * jax.nn.sigmoid(g) * up[j].astype(f32)).astype(bf16)
        for q in range(2):
            acc[q, j // 2] = jnp.zeros(acc.shape[2:], f32)
            flat[q, j // 2] = jnp.zeros(flat.shape[2:], f32)
        return carry

    lax.fori_loop(0, local, prepare, 0)

    def pass_on(s, first, last):
        for n in range(first, last):
            k = lax.rem(e - ranked(en - 2 - n) + en, en)
            along(s, k).wait_recv()
            over(s, k).start()
            mate_own(s, k).start()

    pass_on(0, 0, 1)
    send_own(1)
    pass_on(0, 1, en - 2)
    for copy in sent:
        copy.wait_recv()

    spot = lax.broadcasted_iota(jnp.int32, (total, total), 0)
    lane = lax.broadcasted_iota(jnp.int32, (total, total), 1)
    below = ((spot < lane) & (spot // tokens == lane // tokens)).astype(f32).astype(bf16)
    here = e * local + lax.broadcasted_iota(jnp.int32, (local, total), 0)
    origin = (lax.broadcasted_iota(jnp.int32, (local, total), 1) // tokens * cap).astype(f32)
    top = ids.shape[2]

    def find(which, replica):
        named = jnp.zeros((local, total), f32)
        carried = jnp.zeros((local, total), f32)
        id_all = jnp.concatenate([ids[b, replica] for b in range(en)], axis=1)
        pr_all = jnp.concatenate([probs[b, replica].astype(f32) for b in range(en)], axis=1)
        for k in range(top):
            hit = id_all[k : k + 1, :] == here
            named = jnp.where(hit, 1.0, named)
            carried = jnp.where(hit, pr_all[k : k + 1, :], carried)
        position = jnp.dot(named.astype(bf16), below, preferred_element_type=f32)
        code = jnp.where(named > 0.0, position + origin, -1.0)
        match = code[:, None, :] == lax.broadcasted_iota(jnp.int32, (local, slots, total), 1).astype(f32)
        one[which] = jnp.where(match, 1.0, 0.0).reshape(local * slots, total).astype(bf16)
        return jnp.sum(jnp.where(match, carried[:, None, :], 0.0), axis=2, keepdims=True)

    prob[...] = find(0, d)
    pass_on(0, en - 2, en - 1)
    send_own(2)
    far_send(0, 0).start()
    hs[...] = (prob[...] * hid[...].astype(f32)).astype(bf16)

    def pick(which, src):
        found = jnp.dot(one[which], src, preferred_element_type=f32)
        return found.reshape(local, slots, region).astype(bf16)

    def store_rows(s, p):
        g = index(s, p) - d * steps
        return pltpu.make_async_copy(
            rows.at[s - per, p],
            rows_out.at[:, pl.ds(0, slots), pl.ds(pl.multiple_of(g * region, region), region)],
            lo.at[s - per, p],
        )

    def own_ready(s):
        for k in range(1, en):
            mate_own(s, k).wait_recv()

    def over_ready(s):
        for k in range(1, en):
            mate_over(s, k).wait_recv()

    def relay(s):
        for k in range(1, en):
            over(s, k).wait_recv()
            mate_over(s, k).start()

    def far_relay(q, i):
        far_send(q, i).wait_recv()
        far_mate(q, i).start()

    def turn_0():
        own_ready(0)

    def turn_1():
        send_own(3)
        pass_on(1, 0, en - 1)
        far_send(0, 1).start()
        relay(0)
        far_send(1, 0).start()
        own_ready(1)

    def turn_2():
        pass_on(2, 0, en - 1)
        hid_send().start()
        over_ready(0)

    def turn_3():
        relay(1)
        own_ready(2)

    def turn_4():
        pass_on(3, 0, en - 1)
        over_ready(1)
        far_relay(0, 0)

    def turn_5():
        relay(2)
        own_ready(3)
        far_relay(0, 1)
        far_over().start()

    def turn_6():
        relay(3)
        over_ready(2)

    def turn_7():
        over_ready(3)
        far_relay(1, 0)

    turns = [turn_0, turn_1, turn_2, turn_3, turn_4, turn_5, turn_6, turn_7]

    def step(r, carry):
        s, own = turn(r)
        plane_now = jnp.where(own, plane, 1 - plane)
        slot = lax.rem(r, RING)
        for n, arrive in enumerate(turns):
            pl.when(r == n)(arrive)
        weights(r).wait()
        into = rows.at[lax.rem(s, per), plane_now]
        into[...] = pick(0, tok[index(s, plane_now)])

        @pl.when(s >= per)
        def _():
            store_rows(s, plane_now).start()

        def product(a, b):
            return lax.dot_general(a, b, (((1,), (1,)), ((), ())), preferred_element_type=f32)

        def two_experts(i, carry):
            for q in range(2):
                cols = slice(q * piece, (q + 1) * piece)
                acc[q, i] += product(wbuf[slot, 2 * i, :, cols], into[2 * i, :, cols])
            for q in range(2):
                cols = slice(q * piece, (q + 1) * piece)
                flat[q, i] += product(into[2 * i + 1, :, cols], wbuf[slot, 2 * i + 1, :, cols])
            return carry

        lax.fori_loop(0, local // 2, two_experts, 0, unroll=True)

        @pl.when(r + RING < 2 * steps)
        def _():
            weights(r + RING).start()

        return carry

    lax.fori_loop(0, 2 * steps, step, 0)

    far_over().wait_recv()
    far_mate(1, per - 1).start()
    column = lax.broadcasted_iota(jnp.int32, (slots, cells.shape[2]), 1)

    def finish(i, dots):
        for j, grad in ((2 * i, (acc[0, i] + acc[1, i]).T), (2 * i + 1, flat[0, i] + flat[1, i])):
            gh[j] = grad
            dot = jnp.sum(grad * hid[j].astype(f32), axis=1, keepdims=True)
            dots = jnp.where(column == j, dot, dots)
        return dots

    dots = lax.fori_loop(0, local // 2, finish, jnp.zeros(column.shape, f32), unroll=True)
    for b in range(en):
        cells[b, pl.ds(0, cap), :] = dots[b * cap : (b + 1) * cap, :]
        cells[b, pl.ds(cap, cells.shape[1] - cap), :] = jnp.zeros((cells.shape[1] - cap, cells.shape[2]), f32)
    returns = [
        remote(cells.at[peer[1]], back.at[t, e], rs.at[i], rr.at[i], peer) for i, peer in enumerate(group)
    ]
    for copy in returns:
        copy.start()
    keep = pltpu.make_async_copy(cells.at[e], back.at[t, e], la.at[0])
    keep.start()
    outs = [
        pltpu.make_async_copy(hs, hs_out.at[:, pl.ds(0, slots), :], lx.at[steps]),
        pltpu.make_async_copy(grad_gate, gate_out, lm.at[0]),
        pltpu.make_async_copy(grad_up, up_out, lm.at[1]),
    ]
    outs[0].start()

    def activations(j, carry):
        g = gate[j].astype(f32)
        u = up[j].astype(f32)
        s = jax.nn.sigmoid(g)
        weighted = prob[j] * gh[j]
        grad_up[j] = (weighted * (g * s)).astype(bf16)
        grad_gate[j] = (weighted * u * s * (1.0 + g * (1.0 - s))).astype(bf16)
        return carry

    lax.fori_loop(0, local, activations, 0, unroll=4)
    find(1, far)
    for copy in outs[1:]:
        copy.start()
    far_outs = []
    for i in range(steps):
        far_mate(i // per, i % per).wait_recv()
        q = (plane if i < per else 1 - plane) * per + i % per
        far_rows[q] = pick(1, oth[q])
        far_outs.append(
            pltpu.make_async_copy(
                far_rows.at[q],
                rows_out.at[:, pl.ds(slots, slots), pl.ds(pl.multiple_of(q * region, region), region)],
                lx.at[i],
            )
        )
        far_outs[-1].start()
    hid_send().wait_recv()
    copy = pltpu.make_async_copy(hs_far, hs_out.at[:, pl.ds(slots, slots), :], la.at[1])
    copy.start()
    outs.append(copy)

    def drain(s, carry):
        for k in range(1, en):
            along(s, k).wait_send()
            over(s, k).wait_send()
            mate_own(s, k).wait_send()
            mate_over(s, k).wait_send()
        return carry

    lax.fori_loop(0, steps, drain, 0)
    for copy in sent:
        copy.wait_send()
    hid_send().wait_send()
    for i in range(per):
        for p in range(2):
            far_send(p, i).wait_send()
            far_mate(p, i).wait_send()
            store_rows(per + i, p).wait()
    for copy in returns:
        copy.wait()
    for copy in outs + far_outs + [keep]:
        copy.wait()


def weight_kernel(
    cap, chunk, rows_ref, hs_ref, gate_ref, up_ref, back_ref, ids_ref,
    gate_out, up_out, w_out, probs_out,
    rows, hs, back, ids, grad_gate, grad_up, grad_w, grad_probs,
    sm, sr, sh, so, sg,
):
    f32, bf16 = jnp.float32, jnp.bfloat16
    local = rows.shape[0]
    count = local // chunk

    def part(ref, c):
        return ref.at[pl.ds(c * chunk, chunk)]

    def load(c):
        return pltpu.make_async_copy(part(rows_ref, c), part(rows, c), sr.at[c])

    def load_hs(c):
        return pltpu.make_async_copy(part(hs_ref, c), part(hs, c), sh.at[c])

    def store(j):
        return pltpu.make_async_copy(grad_w.at[j], w_out.at[j], so.at[j])

    small = [(back_ref, back), (ids_ref, ids), (gate_ref, grad_gate), (up_ref, grad_up)]
    small = [pltpu.make_async_copy(a, b, sm.at[n]) for n, (a, b) in enumerate(small)]
    load_hs(0).start()
    load(0).start()
    ends = [
        pltpu.make_async_copy(grad_probs, probs_out, sg.at[0]),
        pltpu.make_async_copy(grad_gate, gate_out.at[0], sg.at[1]),
        pltpu.make_async_copy(grad_up, up_out.at[0], sg.at[2]),
    ]
    load_hs(0).wait()
    load(0).wait()
    for c in range(1, count):
        load_hs(c).start()
        load(c).start()
    for copy in small:
        copy.start()

    def one_chunk(c, carry):
        @pl.when(c > 0)
        def _():
            load_hs(c).wait()
            load(c).wait()

        @pl.when(c == count - 1)
        def _():
            small[2].wait()
            small[3].wait()
            ends[1].start()
            ends[2].start()

        for k in range(chunk):
            j = c * chunk + k
            turned = hs[j].astype(f32).T.astype(bf16)
            grad_w[j] = jnp.dot(turned, rows[j], preferred_element_type=f32).astype(bf16)
            store(j).start()

        return carry

    lax.fori_loop(0, count, one_chunk, 0)

    small[0].wait()
    small[1].wait()
    top, tokens = ids.shape
    tn, en = back.shape[0], back.shape[1]
    summed = back[0]
    for i in range(1, tn):
        summed = summed + back[i]
    cell = jnp.concatenate([summed[b].T[:local] for b in range(en)], axis=0)
    every = lax.broadcasted_iota(jnp.int32, (en * local, tokens), 0)
    spot = lax.broadcasted_iota(jnp.int32, (tokens, tokens), 0)
    lane = lax.broadcasted_iota(jnp.int32, (tokens, tokens), 1)
    below = (spot < lane).astype(f32).astype(bf16)
    named = jnp.zeros(every.shape, f32)
    for k in range(top):
        named = jnp.where(ids[k : k + 1, :] == every, 1.0, named)
    before = jnp.dot(named.astype(bf16), below, preferred_element_type=f32)
    value = jnp.zeros(every.shape, f32)
    for p in range(cap):
        value = jnp.where(before == float(p), cell[:, p : p + 1], value)
    for k in range(top):
        found = jnp.where(ids[k : k + 1, :] == every, value, 0.0)
        grad_probs[k : k + 1, :] = jnp.sum(found, axis=0, keepdims=True)
    ends[0].start()

    def stored(j, carry):
        store(j).wait()
        return carry

    lax.fori_loop(0, local, stored, 0)
    for copy in ends:
        copy.wait()


def on_device(grad_out, route_ids, route_probs, gate_act, up_act, w_down):
    tokens, width = grad_out.shape
    top = route_ids.shape[1]
    tn, en, rn = lax.axis_size("tensor"), lax.axis_size("expert"), lax.axis_size("dp")
    local, units, slots = w_down.shape[0], w_down.shape[1], gate_act.shape[2]
    cap = slots // en
    half = width // rn
    steps = 4
    per = steps // 2
    region = width // (2 * steps)
    total = en * tokens
    f32, bf16 = jnp.float32, jnp.bfloat16
    sem = pltpu.SemaphoreType.DMA
    anyspace = pl.BlockSpec(memory_space=pl.ANY)
    ids_turned = route_ids.T
    both = rn * slots
    hidden_shape = (local, slots, units)
    rows, hs, early_gate, early_up, back = pl.pallas_call(
        functools.partial(gather_kernel, (tn, en, rn), cap),
        out_shape=(
            jax.ShapeDtypeStruct((local, both, half), bf16),
            jax.ShapeDtypeStruct((local, both, units), bf16),
            jax.ShapeDtypeStruct(hidden_shape, bf16),
            jax.ShapeDtypeStruct(hidden_shape, bf16),
            jax.ShapeDtypeStruct((tn, en, 8, 128), f32),
        ),
        in_specs=[anyspace] * 6,
        out_specs=(anyspace,) * 5,
        scratch_shapes=[
            pltpu.VMEM((2 * steps, total, region), bf16),
            pltpu.VMEM((steps, total, region), bf16),
            pltpu.VMEM((en, rn, top, tokens), jnp.int32),
            pltpu.VMEM((en, rn, top, tokens), bf16),
            pltpu.VMEM(hidden_shape, bf16),
            pltpu.VMEM(hidden_shape, bf16),
            pltpu.VMEM((RING, local, units, region), bf16),
            pltpu.VMEM((per, 2, local, slots, region), bf16),
            pltpu.VMEM((steps, local, slots, region), bf16),
            pltpu.VMEM((rn, local * slots, total), bf16),
            pltpu.VMEM((2, local // 2, units, slots), f32),
            pltpu.VMEM((2, local // 2, slots, units), f32),
            pltpu.VMEM(hidden_shape, f32),
            pltpu.VMEM(hidden_shape, bf16),
            pltpu.VMEM(hidden_shape, bf16),
            pltpu.VMEM(hidden_shape, bf16),
            pltpu.VMEM(hidden_shape, bf16),
            pltpu.VMEM(hidden_shape, bf16),
            pltpu.VMEM((local, slots, 1), f32),
            pltpu.VMEM((en, 8, 128), f32),
            sem((2 * steps,)), sem((2,)), sem((2,)), sem((RING,)), sem((per, 2)),
            sem((steps, en - 1)), sem((steps, en - 1)),
            sem((2, en * rn - 1)), sem((2, en * rn - 1)),
            sem((steps, en - 1)), sem((steps, en - 1)),
            sem((steps, en - 1)), sem((steps, en - 1)),
            sem((steps, en - 1)), sem((steps, en - 1)),
            sem((2, per)), sem((2, per)), sem((2, per)), sem((2, per)),
            sem((2,)), sem((tn * en - 1,)), sem((tn * en - 1,)),
        ],
        compiler_params=pltpu.CompilerParams(
            collective_id=0, has_side_effects=True, vmem_limit_bytes=67043328
        ),
    )(grad_out, ids_turned, route_probs.T, gate_act, up_act, w_down)

    chunk = 8
    grad_gate, grad_up, grad_w, grad_probs = pl.pallas_call(
        functools.partial(weight_kernel, cap, chunk),
        in_specs=[anyspace] * 6,
        out_specs=(anyspace,) * 4,
        out_shape=(
            jax.ShapeDtypeStruct((1,) + hidden_shape, bf16),
            jax.ShapeDtypeStruct((1,) + hidden_shape, bf16),
            jax.ShapeDtypeStruct((local, units, half), bf16),
            jax.ShapeDtypeStruct((top, tokens), f32),
        ),
        scratch_shapes=[
            pltpu.VMEM((local, both, half), bf16),
            pltpu.VMEM((local, both, units), bf16),
            pltpu.VMEM((tn, en, 8, 128), f32),
            pltpu.VMEM((top, tokens), jnp.int32),
            pltpu.VMEM(hidden_shape, bf16),
            pltpu.VMEM(hidden_shape, bf16),
            pltpu.VMEM((local, units, half), bf16),
            pltpu.VMEM((top, tokens), f32),
            sem((4,)), sem((local // chunk,)), sem((local // chunk,)), sem((local,)), sem((3,)),
        ],
        compiler_params=pltpu.CompilerParams(vmem_limit_bytes=67043328),
    )(rows, hs, early_gate, early_up, back, ids_turned)
    return grad_gate, grad_up, grad_w, grad_probs.T


def solution(mesh):
    sizes = mesh.shape
    small = sizes["tensor"] == 4 and sizes["dp"] == 2 and sizes["expert"] <= 8
    placed = (
        P(("expert", "dp"), None),
        P(("expert", "dp"), None),
        P(("expert", "dp"), None),
        P("dp", "expert", None, "tensor"),
        P("dp", "expert", None, "tensor"),
        P("expert", "tensor", None),
    )
    return jax.shard_map(
        on_device if small else on_device_wide,
        mesh=mesh,
        in_specs=placed,
        out_specs=(
            P("dp", "expert", None, "tensor"),
            P("dp", "expert", None, "tensor"),
            P("expert", "tensor", "dp"),
            P(("expert", "dp"), None),
        ),
        check_vma=False,
    )
```
